32 devices in a mesh: seq: 8 (over z, x), dp: 4 (over y, core).
Axes of the slice: x: 2, y: 2, z: 4, core: 2. Of those that a mesh axis runs over, the one named last changes fastest.
Arguments:
- layer_input: bfloat16 [4096, 2560], P(('dp', 'seq')), may hold values from -6 to 6
- ssm_input: bfloat16 [4096, 2560], P(('dp', 'seq')), may hold values from -6 to 6
- out_grad: bfloat16 [4096, 2560], P(('dp', 'seq')), may hold values from -6 to 6
- b_weight: bfloat16 [2560, 128], replicated, may hold values from -0.125 to 0.125
- c_weight: bfloat16 [2560, 128], replicated, may hold values from -0.125 to 0.125
- dt_weight: bfloat16 [2560, 40], replicated, may hold values from -0.25 to 0.25
- dt_bias: float32 [40], replicated, may hold values from -9.7 to -8.2
- a_log: float32 [40], replicated, may hold values from -13 to 4.7
- d_skip: float32 [40], replicated, may hold values from 0.5 to 1.5
Outputs:
- grad_ssm_input: bfloat16 [4096, 2560], P(('dp', 'seq'))
- grad_layer_input: bfloat16 [4096, 2560], P(('dp', 'seq'))
- grad_b_weight: float32 [2560, 128], P('seq')
- grad_c_weight: float32 [2560, 128], P('seq')
- grad_dt_weight: float32 [2560, 40], P('seq')
- grad_dt_bias: float32 [40], replicated
- grad_a_log: float32 [40], replicated
- grad_d_skip: float32 [40], replicated
The draws below stay inside these ranges and needn't reach their ends.
All inputs are finite; a program needn't handle non-finite values.
Results may differ from the reference program's by a relative error of at most 0.0018.
Values sent between devices are 32-bit elements; how exact they have to be, the bound alone decides.
No kernel may reach another device: no remote copies, remote signals or barrier semaphores. Data moves between devices by JAX's collectives and lax.ppermute only.
A program may use at most 256 MiB of HBM per device.

```python
import jax
import jax.numpy as jnp
from jax import lax

D_MODEL = 2560
STATE = 128
HEADS = 40
HEAD_DIM = 64
TOK_DEV = 128
SEQLEN = 1024
TOKENS = 4096
N_DP = 4


def decay_setup(key):
    folded = jax.random.fold_in(key, 7)
    streams = jax.random.split(folded, 4)
    portion = 0.5
    retains = jax.random.uniform(streams[0], (HEADS,)) < portion
    slow_rate = jnp.exp(jax.random.uniform(streams[1], (HEADS,), minval=jnp.log(0.3), maxval=jnp.log(2.0))) / SEQLEN
    fast_rate = jnp.exp(jax.random.uniform(streams[2], (HEADS,), minval=jnp.log(1.0 / 50), maxval=jnp.log(1.0 / 20)))
    wanted = jnp.where(retains, slow_rate, fast_rate)
    typical = 0.001 * jnp.exp(jax.random.uniform(streams[3], (HEADS,), minval=-0.7, maxval=0.7))
    return (jnp.log(typical) - 2.0, jnp.log(wanted / typical))


def draw_dt_bias(key, part):
    return decay_setup(key)[0].astype(jnp.float32)


def draw_a_log(key, part):
    return decay_setup(key)[1].astype(jnp.float32)


def raised(values, key, source, target, shards_of, factor):
    def block_of(axis_at):
        return (jnp.arange(values.shape[axis_at]) // (values.shape[axis_at] // shards_of)).reshape((-1,) + (1,) * (values.ndim - 1 - axis_at))

    first = jax.random.permutation(key, shards_of)[block_of(target)]
    other_side = (block_of(target) + shards_of // 2) % shards_of
    return jnp.where((block_of(source) == first) | (block_of(source) == other_side), factor * values, values)


def block_scale(rng, dims, cuts, low, largest):
    def one(dim, blocks):
        heights = jax.random.uniform(jax.random.fold_in(jax.random.fold_in(rng, 6), dim), (blocks,), jnp.float32, low / len(cuts), largest / len(cuts))
        return jnp.repeat(jnp.exp(heights), dims[dim] // blocks).reshape((-1,) + (1,) * (len(dims) - dim - 1))

    factor_of = one(*cuts[0])
    for cut in cuts[1:]:
        factor_of = factor_of * one(*cut)
    return factor_of


def centred(stream_key, dims, width, bound, cuts=(), held_as=jnp.bfloat16):
    entries = width * jax.random.normal(stream_key, dims, jnp.float32)
    if cuts:
        entries = entries * block_scale(stream_key, dims, cuts, -0.22, 0.18)
    return jnp.clip(entries, -bound, bound).astype(held_as)


def bell_draw_with(own_key, shape, scale, bound, cuts, heavy, kind=jnp.bfloat16):
    drawn = scale * jax.random.normal(own_key, shape, jnp.float32)
    if cuts:
        drawn = drawn * block_scale(own_key, shape, cuts, -0.22, 0.18)
    return jnp.clip(raised(drawn, jax.random.fold_in(own_key, 3), *heavy), -bound, bound).astype(kind)


def setup_inputs(seed: int = 0) -> dict:
    key_of = jax.random.split(jax.random.key(seed), 10)
    layer_input = bell_draw_with(key_of[0], (TOKENS, D_MODEL), 1.0, 6.0, ((0, 32),), (0, 1, 32, 2.75))
    ssm_input = centred(key_of[1], (TOKENS, HEADS * HEAD_DIM), 1.0, 6.0, ((0, 32),))
    out_grad = centred(key_of[2], (TOKENS, HEADS * HEAD_DIM), 1.0, 6.0, ((0, 32),))
    b_weight = centred(key_of[3], (D_MODEL, STATE), D_MODEL ** -0.5, 0.125)
    c_weight = centred(key_of[4], (D_MODEL, STATE), D_MODEL ** -0.5, 0.125)
    dt_weight = centred(key_of[5], (D_MODEL, HEADS), (D_MODEL // 4) ** -0.5, 0.25)
    dt_bias = draw_dt_bias(jax.random.fold_in(key_of[9], 71), 0)
    a_log = draw_a_log(jax.random.fold_in(key_of[9], 71), 0)
    d_skip = jnp.clip(jax.random.uniform(key_of[8], (HEADS,), jnp.float32, 0.5, 1.5), 0.5, 1.5)
    return {"layer_input": layer_input, "ssm_input": ssm_input, "out_grad": out_grad, "b_weight": b_weight, "c_weight": c_weight, "dt_weight": dt_weight, "dt_bias": dt_bias, "a_log": a_log, "d_skip": d_skip}


EXACT = lax.Precision.HIGHEST

def block_step(carried, pieces, decay_rate, d_skip):
    proj_b, proj_c, dt_values, inputs = pieces
    length = dt_values.shape[0]
    log_decay = dt_values * decay_rate[None, :]
    cumulative = jnp.cumsum(log_decay, axis=0)
    row_index = lax.broadcasted_iota(jnp.int32, (length, length), 0)
    col_index = lax.broadcasted_iota(jnp.int32, (length, length), 1)
    causal = row_index >= col_index
    spread = cumulative.T[:, :, None] - cumulative.T[:, None, :]
    decay_table = jnp.exp(jnp.where(causal[None], spread, -1e+30))
    scores = jnp.dot(proj_c, proj_b.T, precision=EXACT)
    inner = jnp.einsum('hts,ts,sh,shp->thp', decay_table, scores, dt_values, inputs, precision=EXACT)
    outer = jnp.exp(cumulative)[:, :, None] * jnp.einsum('hpn,tn->thp', carried, proj_c, precision=EXACT)
    block_out = inner + outer + d_skip[None, :, None] * inputs
    block_decay = cumulative[-1]
    weights = jnp.exp(block_decay[None, :] - cumulative) * dt_values
    next_state = jnp.exp(block_decay)[:, None, None] * carried + jnp.einsum('sh,shp,sn->hpn', weights, inputs, proj_b, precision=EXACT)
    return (next_state, block_out)

def replica_forward(u_wide, x_wide, b_wide, c_wide, dt_wide, dt_bias, a_log, d_skip):
    proj_b = jnp.dot(u_wide, b_wide, precision=EXACT)
    proj_c = jnp.dot(u_wide, c_wide, precision=EXACT)
    dt_values = jax.nn.softplus(jnp.dot(u_wide, dt_wide, precision=EXACT) + dt_bias[None, :])
    decay_rate = -jnp.exp(a_log)
    block_count = SEQLEN // TOK_DEV
    pieces = (proj_b.reshape(block_count, TOK_DEV, STATE), proj_c.reshape(block_count, TOK_DEV, STATE), dt_values.reshape(block_count, TOK_DEV, HEADS), x_wide.reshape(block_count, TOK_DEV, HEADS, HEAD_DIM))
    zero_state = jnp.zeros((HEADS, HEAD_DIM, STATE), jnp.float32)

    def advance(carried, block_pieces):
        return block_step(carried, block_pieces, decay_rate, d_skip)
    final_state, outputs = lax.scan(advance, zero_state, pieces)
    return outputs.reshape(SEQLEN, HEADS * HEAD_DIM)

def reference(layer_input, ssm_input, out_grad, b_weight, c_weight, dt_weight, dt_bias, a_log, d_skip):
    b_wide = b_weight.astype(jnp.float32)
    c_wide = c_weight.astype(jnp.float32)
    dt_wide = dt_weight.astype(jnp.float32)
    u_all = layer_input.reshape(N_DP, SEQLEN, D_MODEL)
    x_all = ssm_input.reshape(N_DP, SEQLEN, HEADS * HEAD_DIM)
    g_all = out_grad.reshape(N_DP, SEQLEN, HEADS * HEAD_DIM)

    def replica_grads(replica):
        u_rows, x_rows, g_rows = replica
        primal, pullback = jax.vjp(replica_forward, u_rows.astype(jnp.float32), x_rows.astype(jnp.float32), b_wide, c_wide, dt_wide, dt_bias, a_log, d_skip)
        return pullback(g_rows.astype(jnp.float32))
    results = lax.map(replica_grads, (u_all, x_all, g_all))
    grad_u = results[0].reshape(TOKENS, D_MODEL).astype(jnp.bfloat16)
    grad_x = results[1].reshape(TOKENS, HEADS * HEAD_DIM).astype(jnp.bfloat16)
    return (grad_x, grad_u, lax.optimization_barrier(jnp.sum(results[2], axis=0)), lax.optimization_barrier(jnp.sum(results[3], axis=0)), lax.optimization_barrier(jnp.sum(results[4], axis=0)), lax.optimization_barrier(jnp.sum(results[5], axis=0)), lax.optimization_barrier(jnp.sum(results[6], axis=0)), lax.optimization_barrier(jnp.sum(results[7], axis=0)))
```

```python
import jax
import jax.numpy as jnp
from jax import lax
from jax.experimental import pallas as pl
from jax.experimental.pallas import tpu as pltpu
from jax.sharding import PartitionSpec as P

F32 = jnp.float32
BF16 = jnp.bfloat16
LANES = 128
CHUNKS = 2

NN = (((1,), (0,)), ((), ()))
NT = (((1,), (1,)), ((), ()))
TN = (((0,), (0,)), ((), ()))


def mm(a, b, dims):
    return lax.dot_general(a, b, dims, preferred_element_type=F32)


def split2(a):
    hi = a.astype(BF16)
    return hi, (a - hi.astype(F32)).astype(BF16)


def split3(a):
    hi = a.astype(BF16)
    rest = a - hi.astype(F32)
    mid = rest.astype(BF16)
    return hi, mid, (rest - mid.astype(F32)).astype(BF16)


def dot3(a, b, dims):
    ah, al = split2(a)
    bh, bl = split2(b)
    return mm(ah, bh, dims) + (mm(ah, bl, dims) + mm(al, bh, dims))


def dot_left(a, b, dims):
    ah, al = split2(a)
    return mm(ah, b, dims) + mm(al, b, dims)


def dot_left_full(a, b, dims):
    ah, am, al = split3(a)
    return mm(ah, b, dims) + (mm(am, b, dims) + mm(al, b, dims))


def dot_right_full(a, b, dims):
    bh, bm, bl = split3(b)
    return mm(a, bh, dims) + (mm(a, bm, dims) + mm(a, bl, dims))


def iota(shape, axis):
    return lax.broadcasted_iota(jnp.int32, shape, axis)


def log1p_unit(y):
    s = y / (2.0 + y)
    q = s * s
    poly = jnp.full_like(q, 1.0 / 17)
    for k in (15, 13, 11, 9, 7, 5, 3, 1):
        poly = poly * q + 1.0 / k
    return 2.0 * s * poly


def triangle(length, lower):
    r, c = iota((length, length), 0), iota((length, length), 1)
    keep = (r >= c) if lower else (c >= r)
    return jnp.where(keep, 1.0, 0.0).astype(BF16)


def expand_matrix(head_start, width, lanes):
    r, c = iota((LANES, lanes), 0), iota((LANES, lanes), 1)
    return jnp.where(r == head_start + c // width, 1.0, 0.0).astype(BF16)


def collect_matrix(head_start, width, lanes):
    r, c = iota((lanes, LANES), 0), iota((lanes, LANES), 1)
    return jnp.where(c == head_start + r // width, 1.0, 0.0).astype(BF16)


def coefficients(tile, heads_all, heads_half):
    lane = iota(tile.shape, 1) < heads_half
    length = tile.shape[0]
    dt = jnp.where(lane, tile, 0.0)
    cum = jnp.where(lane, pltpu.roll(tile, LANES - heads_all, 1), 0.0)
    last = cum[length - 1 : length, :]
    from_start = jnp.where(lane, jnp.exp(cum), 0.0)
    to_end = jnp.where(lane, jnp.exp(last - cum), 0.0)
    decay = jnp.where(lane[:1], jnp.exp(last), 0.0)
    return dt, cum, from_start, to_end, decay


def row_of(v, rows=8):
    return jnp.broadcast_to(v, (rows, v.shape[1]))


def proj_kernel(at_ref, u_ref, wb_ref, wc_ref, wd_ref, bias_ref, alog_ref, own_ref, snd_ref, *, heads):
    length = u_ref.shape[0]
    state = wb_ref.shape[1]
    u = u_ref[...]
    b = mm(u, wb_ref[...], NN)
    c = mm(u, wc_ref[...], NN)
    raw = mm(u, wd_ref[...], NN) + bias_ref[...]
    dt = jnp.maximum(raw, 0.0) + log1p_unit(jnp.exp(-jnp.abs(raw)))
    sig = 1.0 / (1.0 + jnp.exp(-raw))
    log_decay = dt * -jnp.exp(alog_ref[...])
    cum = dot_right_full(triangle(length, True), log_decay, NN)
    lane = iota(raw.shape, 1)
    tile = jnp.where(lane < heads, dt, jnp.where(lane < 2 * heads, cum, sig))
    half = heads // 2
    at = at_ref[0]
    own_ref[:, :state] = b
    own_ref[:, state : 2 * state] = c
    own_ref[:, 2 * state :] = pltpu.roll(tile, (LANES - half * at) % LANES, 1)
    snd_ref[:, :state] = b
    snd_ref[:, state : 2 * state] = c
    snd_ref[:, 2 * state :] = pltpu.roll(tile, (LANES - half * (1 - at)) % LANES, 1)


def state_kernel(
    at_ref, xo_ref, go_ref, xgr_ref, po_ref, pr_ref, p_ref, q_ref, sf_ref, gs_ref, d_ref, *, heads, width, start
):
    half = heads // 2
    state = (po_ref.shape[1] - LANES) // 2
    lanes = xo_ref.shape[1]
    spread = expand_matrix(start, width, lanes)
    first_is_own = at_ref[0] == 0

    def local(x, g, pack_ref):
        dt, cum, from_start, to_end, decay = coefficients(pack_ref[:, 2 * state :], heads, half)
        xw = x * dot_left(to_end * dt, spread, NN)
        gw = g * dot_left(from_start, spread, NN)
        s = dot3(pack_ref[:, :state], xw, TN)
        back = dot3(pack_ref[:, state : 2 * state], gw, TN)
        return s, back, dot_left_full(row_of(decay), spread, NN)

    s_own, b_own, d_own = local(xo_ref[...].astype(F32), go_ref[...].astype(F32), po_ref)
    s_rcv, b_rcv, d_rcv = local(xgr_ref[0], xgr_ref[1], pr_ref)

    def pick(a, b):
        return jnp.where(first_is_own, a, b)

    s_first, s_second = pick(s_own, s_rcv), pick(s_rcv, s_own)
    b_first, b_second = pick(b_own, b_rcv), pick(b_rcv, b_own)
    d_first, d_second = pick(d_own, d_rcv), pick(d_rcv, d_own)
    p_ref[...] = d_second[:1] * s_first + s_second
    q_ref[...] = d_first[:1] * b_second + b_first
    sf_ref[...] = s_first
    gs_ref[...] = b_second
    d_ref[...] = d_first * d_second


def intra_kernel(
    xo_ref, go_ref, *refs, heads, width, chunks
):
    xgr_refs = refs[:chunks]
    po_ref, pr_ref = refs[chunks : chunks + 2]
    back_ref, gbc_ref, rows_ref = refs[chunks + 2 : chunks + 5]
    x_ref, g_ref, cumt_ref, acc_ref = refs[chunks + 5 :]
    length, lanes = xo_ref.shape
    half = heads // 2
    state = (po_ref.shape[1] - LANES) // 2
    part = lanes // chunks
    x_ref[0] = xo_ref[...]
    g_ref[0] = go_ref[...]
    for j in range(chunks):
        x_ref[1, :, j * part : (j + 1) * part] = xgr_refs[j][0].astype(BF16)
        g_ref[1, :, j * part : (j + 1) * part] = xgr_refs[j][1].astype(BF16)
    src, dst = iota((length, length), 0), iota((length, length), 1)
    causal = dst >= src
    low = iota((length, LANES), 1) < width
    for which, pack_ref in ((0, po_ref), (1, pr_ref)):
        b = pack_ref[:, :state]
        c = pack_ref[:, state : 2 * state]
        tile = pack_ref[:, 2 * state :]
        scores = dot3(b, c, NT)
        cumt_ref[...] = jnp.transpose(pltpu.roll(tile, LANES - heads, 1))
        acc_ref[...] = jnp.zeros_like(acc_ref)

        def step(k, _):
            at = pl.multiple_of(k * LANES, LANES)
            xp = x_ref[which, :, pl.ds(at, LANES)]
            gp = g_ref[which, :, pl.ds(at, LANES)]
            zero = jnp.zeros_like(xp)
            x2 = jnp.concatenate([jnp.where(low, xp, zero), jnp.where(low, zero, xp)], axis=0)
            g2 = jnp.concatenate([jnp.where(low, gp, zero), jnp.where(low, zero, gp)], axis=0)
            dots = mm(x2, gp, NT)
            turned = pltpu.roll(tile, LANES - 2 * k, 1)
            his, los = [], []
            total = acc_ref[...]
            for e in range(2):
                h = 2 * k + e
                dt_col = jnp.broadcast_to(turned[:, e : e + 1], (length, length))
                cum_col = jnp.broadcast_to(turned[:, heads + e : heads + e + 1], (length, length))
                cum_row = cumt_ref[pl.ds(h, 1), :]
                table = jnp.exp(jnp.where(causal, cum_row - cum_col, -1e30))
                pairs = table * dots[e * length : (e + 1) * length] * dt_col
                total = total + pairs
                rows_ref[which, pl.ds(h, 1), :] = jnp.sum(pairs * scores, axis=0, keepdims=True)
                hi, lo = split2(table * scores)
                his.append(hi)
                los.append(lo)
            acc_ref[...] = total
            back = mm(jnp.concatenate(his, axis=1), g2, NN) + mm(jnp.concatenate(los, axis=1), g2, NN)
            back_ref[which, :, pl.ds(at, LANES)] = back
            return 0

        rows_ref[which] = jnp.zeros(rows_ref.shape[1:], F32)
        lax.fori_loop(0, lanes // LANES, step, 0)
        pair_sum = acc_ref[...]
        gbc_ref[which, :, :state] = dot3(pair_sum, c, NN)
        gbc_ref[which, :, state:] = dot3(pair_sum, b, TN)


def carry_kernel(
    at_ref, xo_ref, go_ref, *refs, heads, width, chunks
):
    xgr_refs = refs[:chunks]
    sf_refs = refs[chunks : 2 * chunks]
    gs_refs = refs[2 * chunks : 3 * chunks]
    ci_refs = refs[3 * chunks : 4 * chunks]
    co_refs = refs[4 * chunks : 5 * chunks]
    po_ref, pr_ref, back_ref, gbc_ref, rows_ref, skip_ref, rate_ref = refs[5 * chunks : 5 * chunks + 7]
    gxo_ref, gxs_ref, pko_ref, pks_ref, extra_ref = refs[5 * chunks + 7 :]
    length, all_lanes = xo_ref.shape
    half = heads // 2
    state = (po_ref.shape[1] - LANES) // 2
    lanes = all_lanes // chunks
    own_first = at_ref[0] == 0
    rate = rate_ref[...]
    packs = (po_ref, pr_ref)
    co = [coefficients(r[:, 2 * state :], heads, half) for r in packs]
    zeros = jnp.zeros((length, LANES), F32)
    gb, gc = [gbc_ref[w, :, :state] for w in (0, 1)], [gbc_ref[w, :, state:] for w in (0, 1)]
    r_intra, r_back, r_front = [zeros, zeros], [zeros, zeros], [zeros, zeros]
    cross = [jnp.zeros((8, LANES), F32) for _ in (0, 1)]
    skip_sum = jnp.zeros((8, LANES), F32)
    for j in range(chunks):
        start = j * (half // chunks)
        spread = expand_matrix(start, width, lanes)
        collect = collect_matrix(start, width, lanes)
        cols = slice(j * lanes, (j + 1) * lanes)
        decays = [dot_left_full(row_of(co[w][4]), spread, NN)[:1] for w in (0, 1)]
        cin, cout = ci_refs[j][...], co_refs[j][...]
        d_first = jnp.where(own_first, decays[0], decays[1])
        d_second = jnp.where(own_first, decays[1], decays[0])
        cin_second = d_first * cin + sf_refs[j][...]
        cout_first = d_second * cout + gs_refs[j][...]
        for w in (0, 1):
            is_first = own_first if w == 0 else jnp.logical_not(own_first)
            my_in = jnp.where(is_first, cin, cin_second)
            my_out = jnp.where(is_first, cout_first, cout)
            dt, cum, from_start, to_end, decay = co[w]
            if w == 0:
                x, g = xo_ref[:, cols].astype(F32), go_ref[:, cols].astype(F32)
            else:
                x, g = xgr_refs[j][0], xgr_refs[j][1]
            b, c = packs[w][:, :state], packs[w][:, state : 2 * state]
            front = dot3(c, my_in, NN)
            back = dot3(b, my_out, NN)
            dt_wide = dot_left(dt, spread, NN)
            te_wide = dot_left(to_end, spread, NN)
            fs_wide = dot_left(from_start, spread, NN)
            intra = back_ref[w, :, cols]
            grad_x = dt_wide * (intra + te_wide * back) + skip_ref[:1, cols] * g
            if w == 0:
                gxo_ref[:, cols] = grad_x.astype(BF16)
            else:
                gxs_ref[:, cols] = grad_x
            r_intra[w] = r_intra[w] + dot_left_full(x * intra, collect, NN)
            r_back[w] = r_back[w] + dot_left_full(x * back, collect, NN)
            r_front[w] = r_front[w] + dot_left_full(g * front, collect, NN)
            gb[w] = gb[w] + dot3(x * (te_wide * dt_wide), my_out, NT)
            gc[w] = gc[w] + dot3(g * fs_wide, my_in, NT)
            both = jnp.sum(my_in * my_out, axis=0, keepdims=True)
            cross[w] = cross[w] + dot_left_full(row_of(both), collect, NN)
            skip_sum = skip_sum + dot_left_full(row_of(jnp.sum(x * g, axis=0, keepdims=True)), collect, NN)
    later = triangle(length, False)
    last_row = iota((length, LANES), 0) == length - 1
    bias_sum = jnp.zeros((1, LANES), F32)
    alog_sum = jnp.zeros((1, LANES), F32)
    lane = iota((length, LANES), 1) < half
    for w, out_ref in ((0, pko_ref), (1, pks_ref)):
        dt, cum, from_start, to_end, decay = co[w]
        sig = pltpu.roll(packs[w][:, 2 * state :], LANES - 2 * heads, 1)
        own_out = to_end * dt * r_back[w]
        change = jnp.transpose(rows_ref[w]) - dt * r_intra[w] + from_start * r_front[w] - own_out
        tail = decay * cross[w][:1] + jnp.sum(own_out, axis=0, keepdims=True)
        change = change + jnp.where(last_row, tail, 0.0)
        grad_log = dot_right_full(later, change, NN)
        direct = r_intra[w] + to_end * r_back[w]
        grad_raw = jnp.where(lane, (direct + grad_log * rate[:1]) * sig, 0.0)
        bias_sum = bias_sum + jnp.sum(grad_raw, axis=0, keepdims=True)
        alog_sum = alog_sum + jnp.sum(grad_log * dt, axis=0, keepdims=True) * rate[:1]
        out_ref[:, :state] = gb[w]
        out_ref[:, state : 2 * state] = gc[w]
        out_ref[:, 2 * state :] = grad_raw
    row = iota((8, LANES), 0)
    extra = jnp.where(row == 0, bias_sum, jnp.where(row == 1, alog_sum, jnp.where(row == 2, skip_sum[:1], 0.0)))
    extra_ref[...] = jnp.where(iota((8, LANES), 1) < half, extra, 0.0)


def join_kernel(at_ref, own_ref, rcv_ref, extra_ref, out_ref, extra_out_ref, *, heads):
    state = (own_ref.shape[1] - LANES) // 2
    half = heads // 2
    at = at_ref[0]
    out_ref[:, : 2 * state] = own_ref[:, : 2 * state] + rcv_ref[:, : 2 * state]
    mine = pltpu.roll(own_ref[:, 2 * state :], half * at, 1)
    other = pltpu.roll(rcv_ref[:, 2 * state :], half * (1 - at), 1)
    out_ref[:, 2 * state :] = mine + other
    extra_out_ref[...] = pltpu.roll(extra_ref[...], half * at, 1)


def merge_kernel(at_ref, own_ref, rcv_ref, out_ref):
    lanes = own_ref.shape[1]
    mine = pl.multiple_of(at_ref[0] * lanes, LANES)
    other = pl.multiple_of((1 - at_ref[0]) * lanes, LANES)
    out_ref[:, pl.ds(mine, lanes)] = own_ref[...]
    out_ref[:, pl.ds(other, lanes)] = rcv_ref[...].astype(BF16)


def grad_u_kernel(cols_ref, wb_ref, wc_ref, wd_ref, out_ref):
    state = wb_ref.shape[1]
    total = dot_left(cols_ref[:, :state], wb_ref[...], NT)
    total = total + dot_left(cols_ref[:, state : 2 * state], wc_ref[...], NT)
    total = total + dot_left(cols_ref[:, 2 * state :], wd_ref[...], NT)
    out_ref[...] = total.astype(BF16)


def weight_kernel(*refs, pieces, heads, state):
    u = jnp.concatenate([r[i].astype(BF16) for r in refs[:pieces] for i in range(r.shape[0])], axis=0)
    cols = jnp.concatenate([r[i] for r in refs[pieces : 2 * pieces] for i in range(r.shape[0])], axis=0)
    extra_ref, out_ref = refs[2 * pieces :]
    count, block, _ = out_ref.shape
    each = (block - heads) // 2
    hi, lo = split2(cols[:, : 2 * state])
    wide = mm(u, hi, TN) + mm(u, lo, TN)
    thi, tlo = split2(cols[:, 2 * state :])
    turned = mm(thi, u, TN) + mm(tlo, u, TN)
    turned = jnp.concatenate([turned[:heads], jnp.zeros((heads, LANES), F32)], axis=1)
    tail = jnp.transpose(jnp.concatenate([extra_ref[...], jnp.zeros((LANES - 8, LANES), F32)], axis=0))
    tail = pltpu.roll(tail, each, 1)[:heads]
    lane = iota((heads, LANES), 1)
    for s in range(count):
        rows = slice(s * each, (s + 1) * each)
        out_ref[s, :each] = wide[rows, :state]
        out_ref[s, each : 2 * each] = wide[rows, state:]
        start = s * each // LANES * LANES
        window = pltpu.roll(turned[:, start : start + 2 * LANES], (2 * LANES + start - s * each) % (2 * LANES), 1)
        out_ref[s, 2 * each :] = jnp.where(lane < each, window[:, :LANES], tail)


def final_kernel(at_ref, *refs, pieces, heads, order):
    parts = [r[i] for r in refs[:pieces] for i in range(r.shape[0])]
    gb_ref, gc_ref, gd_ref, bias_ref, alog_ref, skip_ref = refs[pieces:]
    each = gb_ref.shape[0] // len(parts)
    mine = at_ref[0]
    total = None
    for d in range(len(parts)):
        block = parts[0]
        for part, flip in list(zip(parts, order))[1:]:
            block = jnp.where(mine == d ^ flip, part, block)
        rows = slice(d * each, (d + 1) * each)
        gb_ref[rows] = block[:each]
        gc_ref[rows] = block[each : 2 * each]
        tail = jnp.concatenate([block[2 * each :], jnp.zeros((LANES - heads, LANES), F32)], axis=0)
        turned = jnp.transpose(tail)
        gd_ref[rows] = turned[:each, :heads]
        total = turned if total is None else total + turned
    bias_ref[...] = total[each : each + 1, :heads]
    alog_ref[...] = total[each + 1 : each + 2, :heads]
    skip_ref[...] = total[each + 2 : each + 3, :heads]


def vmem(n):
    return [pl.BlockSpec(memory_space=pltpu.VMEM) for _ in range(n)]


def call(kernel, n_in, outs, scratch=(), flops=10**8, scalar=True, name=None):
    specs = ([pl.BlockSpec(memory_space=pltpu.SMEM)] if scalar else []) + vmem(n_in)
    return pl.pallas_call(
        kernel,
        in_specs=specs,
        out_specs=vmem(len(outs)),
        out_shape=[jax.ShapeDtypeStruct(s, t) for s, t in outs],
        scratch_shapes=list(scratch),
        cost_estimate=pl.CostEstimate(flops=flops, transcendentals=0, bytes_accessed=10**6),
        compiler_params=pltpu.CompilerParams(vmem_limit_bytes=48 << 20),
        name=name,
    )


def body(layer_input, ssm_input, out_grad, b_weight, c_weight, dt_weight, dt_bias, a_log, d_skip):
    import functools

    length, model = layer_input.shape
    heads = dt_bias.shape[0]
    state = b_weight.shape[1]
    width = ssm_input.shape[1] // heads
    half = heads // 2
    lanes = half * width
    part = lanes // CHUNKS
    count = lax.axis_size("seq")
    place = lax.axis_index("seq") % 2
    at = jnp.reshape(place, (1,)).astype(jnp.int32)
    swap = [(i, i ^ 1) for i in range(count)]
    up = [(i, i + 2) for i in range(count - 2)]
    down = [(i + 2, i) for i in range(count - 2)]
    pack = 2 * state + LANES

    def exchange(value):
        return lax.ppermute(value, "seq", swap)

    def half_of(value, which, j=None):
        if j is None:
            return lax.dynamic_slice(value, (0, which * lanes), (length, lanes))
        return lax.dynamic_slice(value, (0, which * lanes + j * part), (length, part))

    groups = lax.axis_size("dp")
    group = lax.axis_index("dp")
    each = model // count // groups
    bits = []
    while groups >> (len(bits) + 1):
        bits.insert(0, 1 << len(bits))

    def spread_pieces(value):
        pieces = [value]
        for bit in bits:
            sent = pieces[0] if len(pieces) == 1 else jnp.concatenate(pieces, axis=0)
            pieces.append(lax.ppermute(sent, "dp", [(d, d ^ bit) for d in range(groups)]))
        return pieces

    def column_pieces(value):
        value = value.reshape(length, count, groups, each).transpose(2, 0, 1, 3)
        pieces = [value.reshape(groups, 1, length, count * each)]
        for bit in bits:
            high = (group // bit) % 2

            def side(piece, which):
                return lax.dynamic_slice_in_dim(piece, which * bit, bit, axis=0)

            sent = jnp.concatenate([side(p, 1 - high).astype(F32) for p in pieces], axis=1)
            pieces = [side(p, high) for p in pieces]
            pieces.append(lax.ppermute(sent, "dp", [(d, d ^ bit) for d in range(groups)]))
        return [p[0] for p in pieces]

    received = []
    for j in range(CHUNKS):
        both = jnp.stack([half_of(v, 1 - place, j).astype(F32) for v in (ssm_input, out_grad)])
        received.append(both)
    tripled = jnp.pad(jnp.concatenate([dt_weight] * 3, axis=1), ((0, 0), (0, LANES - 3 * heads)))

    def row3(v):
        return jnp.pad(jnp.concatenate([v] * 3), (0, LANES - 3 * heads))[None]

    own, send = call(
        functools.partial(proj_kernel, heads=heads), 6, [((length, pack), F32)] * 2, name="proj"
    )(at, layer_input, b_weight, c_weight, tripled, row3(dt_bias), row3(a_log))
    first = exchange(received[0])
    send, *rest = lax.optimization_barrier((send, *received[1:]))
    rcv = exchange(send)
    received = [first] + [exchange(v) for v in rest]
    u_pieces = column_pieces(layer_input)
    x_own, g_own = half_of(ssm_input, place), half_of(out_grad, place)

    carried, locals_ = [], []
    for j in range(CHUNKS):
        p, q, s_first, g_second, decay = call(
            functools.partial(
                state_kernel, heads=heads, width=width, start=j * (half // CHUNKS)
            ),
            5,
            [((state, part), F32)] * 4 + [((8, part), F32)],
            name="state",
        )(at, x_own[:, j * part : (j + 1) * part], g_own[:, j * part : (j + 1) * part], received[j], own, rcv)
        carried.append((p, q, decay[:1]))
        locals_.append((s_first, g_second))
    ins, outs = [], []
    for p, q, decay in carried:
        inward = lax.ppermute(p, "seq", up)
        outward = lax.ppermute(q, "seq", down)
        for _ in range(count // 2 - 2):
            inward = lax.ppermute(p + decay * inward, "seq", up)
            outward = lax.ppermute(q + decay * outward, "seq", down)
        ins.append(inward)
        outs.append(outward)
    back, grad_bc, rows = call(
        functools.partial(intra_kernel, heads=heads, width=width, chunks=CHUNKS),
        4 + CHUNKS,
        [((2, length, lanes), F32), ((2, length, 2 * state), F32), ((2, LANES, length), F32)],
        scratch=[
            pltpu.VMEM((2, length, lanes), BF16),
            pltpu.VMEM((2, length, lanes), BF16),
            pltpu.VMEM((LANES, length), F32),
            pltpu.VMEM((length, length), F32),
        ],
        flops=10**9,
        scalar=False,
        name="intra",
    )(x_own, g_own, *received, own, rcv)

    def my_heads(v):
        return lax.dynamic_slice(v, (place * half,), (half,))

    skip_row = jnp.broadcast_to(jnp.repeat(my_heads(d_skip), width)[None], (8, lanes))
    rate_row = jnp.broadcast_to(jnp.pad(-jnp.exp(my_heads(a_log)), (0, LANES - half))[None], (8, LANES))
    gx_own, gx_send, pack_own, pack_send, extra = call(
        functools.partial(carry_kernel, heads=heads, width=width, chunks=CHUNKS),
        2 + 5 * CHUNKS + 7,
        [
            ((length, lanes), BF16),
            ((length, lanes), F32),
            ((length, pack), F32),
            ((length, pack), F32),
            ((8, LANES), F32),
        ],
        name="carry",
    )(
        at, x_own, g_own, *received,
        *[v[0] for v in locals_], *[v[1] for v in locals_], *ins, *outs,
        own, rcv, back, grad_bc, rows, skip_row, rate_row,
    )
    pack_rcv = exchange(pack_send)
    gx_rcv = exchange(gx_send)
    cols, extra = call(
        functools.partial(join_kernel, heads=heads), 3, [((length, pack), F32), ((8, LANES), F32)], name="join"
    )(at, pack_own, pack_rcv, extra)
    (grad_x,) = call(merge_kernel, 2, [((length, 2 * lanes), BF16)], name="merge")(at, gx_own, gx_rcv)
    gathered = spread_pieces(cols[None])
    (grad_u,) = call(grad_u_kernel, 4, [((length, model), BF16)], scalar=False, name="grad_u")(
        cols, b_weight, c_weight, tripled
    )
    (blocks,) = call(
        functools.partial(weight_kernel, pieces=len(gathered), heads=heads, state=state),
        2 * len(gathered) + 1,
        [((count, 2 * each + heads, LANES), F32)],
        scalar=False,
        name="weights",
    )(*u_pieces, *gathered, extra)
    mine = jnp.sum(lax.all_to_all(blocks, "seq", 0, 0, tiled=True), axis=0, keepdims=True)
    parts = spread_pieces(mine)
    order = [0]
    for bit in bits:
        order = order + [f ^ bit for f in order]
    rows_out = model // count
    gb, gc, gd, bias, alog, skip = call(
        functools.partial(final_kernel, pieces=len(parts), heads=heads, order=order),
        len(parts),
        [((rows_out, state), F32)] * 2 + [((rows_out, heads), F32)] + [((1, heads), F32)] * 3,
        name="final",
    )(jnp.reshape(group, (1,)).astype(jnp.int32), *parts)
    return grad_x, grad_u, gb, gc, gd, bias[0], alog[0], skip[0]


def solution(mesh):
    rows = P(("dp", "seq"), None)
    in_specs = (rows, rows, rows, P(), P(), P(), P(), P(), P())
    out_specs = (rows, rows, P("seq", None), P("seq", None), P("seq", None), P(), P(), P())
    return jax.shard_map(body, mesh=mesh, in_specs=in_specs, out_specs=out_specs, check_vma=False)
```

```python
import functools

import jax
import jax.numpy as jnp
from jax import lax
from jax.experimental import pallas as pl
from jax.experimental.pallas import tpu as pltpu
from jax.sharding import PartitionSpec as P


F32 = jnp.float32
BF16 = jnp.bfloat16
LANES = 128
SHARES = (8, 8, 4)

NN = (((1,), (0,)), ((), ()))
NT = (((1,), (1,)), ((), ()))
TN = (((0,), (0,)), ((), ()))


def mm(a, b, dims):
    return lax.dot_general(a, b, dims, preferred_element_type=F32)


def split2(a):
    hi = a.astype(BF16)
    return hi, (a - hi.astype(F32)).astype(BF16)


def split3(a):
    hi = a.astype(BF16)
    rest = a - hi.astype(F32)
    mid = rest.astype(BF16)
    return hi, mid, (rest - mid.astype(F32)).astype(BF16)


def mm_sum(terms, dims):
    (left,), (right,) = dims[0]
    a = jnp.concatenate([t[0] for t in terms], axis=left)
    b = jnp.concatenate([t[1] for t in terms], axis=right)
    return mm(a, b, dims)


def dot3(a, b, dims):
    ah, al = split2(a)
    bh, bl = split2(b)
    return mm_sum([(al, bh), (ah, bl), (ah, bh)], dims)


def dot_left(a, b, dims):
    ah, al = split2(a)
    return mm_sum([(al, b), (ah, b)], dims)


def dot_left_full(a, b, dims):
    ah, am, al = split3(a)
    return mm_sum([(al, b), (am, b), (ah, b)], dims)


def dot_right_full(a, b, dims):
    bh, bm, bl = split3(b)
    return mm_sum([(a, bl), (a, bm), (a, bh)], dims)


def iota(shape, axis):
    return lax.broadcasted_iota(jnp.int32, shape, axis)


def log1p_unit(y):
    s = y / (2.0 + y)
    q = s * s
    poly = jnp.full_like(q, 1.0 / 17)
    for k in (15, 13, 11, 9, 7, 5, 3, 1):
        poly = poly * q + 1.0 / k
    return 2.0 * s * poly


def triangle(length, lower):
    r, c = iota((length, length), 0), iota((length, length), 1)
    keep = (r >= c) if lower else (c >= r)
    return jnp.where(keep, 1.0, 0.0).astype(BF16)


def expand_matrix(head_start, width, lanes):
    r, c = iota((LANES, lanes), 0), iota((LANES, lanes), 1)
    return jnp.where(r == head_start + c // width, 1.0, 0.0).astype(BF16)


def collect_matrix(head_start, width, lanes):
    r, c = iota((lanes, LANES), 0), iota((lanes, LANES), 1)
    return jnp.where(c == head_start + r // width, 1.0, 0.0).astype(BF16)


def coefficients(tile, heads_all, heads_half):
    lane = iota(tile.shape, 1) < heads_half
    length = tile.shape[0]
    dt = jnp.where(lane, tile, 0.0)
    cum = jnp.where(lane, pltpu.roll(tile, LANES - heads_all, 1), 0.0)
    last = cum[length - 1 : length, :]
    from_start = jnp.where(lane, jnp.exp(cum), 0.0)
    to_end = jnp.where(lane, jnp.exp(last - cum), 0.0)
    decay = jnp.where(lane[:1], jnp.exp(last), 0.0)
    return dt, cum, from_start, to_end, decay


def row_of(v, rows=8):
    return jnp.broadcast_to(v, (rows, v.shape[1]))


def lanes_of(chunk):
    return slice(chunk[0], chunk[0] + chunk[1])


def send_kernel(at_ref, x_ref, g_ref, out_ref, buf_ref, sems, *, half_lanes, start):
    part = out_ref.shape[2]
    first = pl.multiple_of((1 - at_ref[0]) * half_lanes + start, LANES)
    copies = []
    for i, ref in enumerate((x_ref, g_ref)):
        copies.append(pltpu.make_async_copy(ref.at[:, pl.ds(first, part)], buf_ref.at[i], sems.at[i]))
        copies[-1].start()
    for i, copy in enumerate(copies):
        copy.wait()
        out_ref[i] = buf_ref[i].astype(F32)


def keep_kernel(at_ref, x_ref, g_ref, *refs, half_lanes, chunks):
    keeps, sends = refs[:2], refs[2 : 2 + len(chunks)]
    buf_ref, keep_sems, send_sems = refs[2 + len(chunks) :]
    own = pl.multiple_of(at_ref[0] * half_lanes, LANES)
    other = pl.multiple_of((1 - at_ref[0]) * half_lanes, LANES)
    rest = half_lanes - chunks[0][0] if chunks else 0
    sending, keeping = [], []
    for i, ref in enumerate((x_ref, g_ref)):
        if chunks:
            source = ref.at[:, pl.ds(pl.multiple_of(other + chunks[0][0], LANES), rest)]
            sending.append(pltpu.make_async_copy(source, buf_ref.at[i], send_sems.at[i]))
            sending[-1].start()
        keeping.append(pltpu.make_async_copy(ref.at[:, pl.ds(own, half_lanes)], keeps[i], keep_sems.at[i]))
        keeping[-1].start()
    for i, copy in enumerate(sending):
        copy.wait()
        for chunk, out_ref in zip(chunks, sends):
            first = chunk[0] - chunks[0][0]
            out_ref[i] = buf_ref[i, :, first : first + chunk[1]].astype(F32)
    for copy in keeping:
        copy.wait()


def columns_kernel(group_ref, u_ref, keep_ref, send_ref, *, count, groups, each):
    u = u_ref[...].astype(F32)
    taken = []
    for d in range(groups):
        parts = [u[:, (s * groups + d) * each : (s * groups + d + 1) * each] for s in range(count)]
        taken.append(jnp.concatenate(parts, axis=1))
    half = groups // 2
    high = group_ref[2] >= half
    for i in range(half):
        keep_ref[i, 0] = jnp.where(high, taken[half + i], taken[i]).astype(BF16)
        send_ref[i, 0] = jnp.where(high, taken[i], taken[half + i])


def halve_kernel(group_ref, *refs, bit):
    keep_ref, send_ref = refs[-2:]
    high = (group_ref[2] // bit) % 2 == 1
    done = 0
    for ref in refs[:-2]:
        for k in range(ref.shape[1]):
            for i in range(bit):
                low_part, high_part = ref[i, k].astype(F32), ref[bit + i, k].astype(F32)
                keep_ref[i, done + k] = jnp.where(high, high_part, low_part).astype(BF16)
                send_ref[i, done + k] = jnp.where(high, low_part, high_part)
        done += ref.shape[1]


def total_kernel(parts_ref, out_ref):
    total = parts_ref[0]
    for i in range(1, parts_ref.shape[0]):
        total = total + parts_ref[i]
    out_ref[0] = total


def proj_kernel(at_ref, u_ref, wb_ref, wc_ref, wd_ref, rows_ref, own_ref, snd_ref, misc_ref, *, heads):
    length = u_ref.shape[0]
    state = wb_ref.shape[1]
    u = u_ref[...]
    b = mm(u, wb_ref[...], NN)
    c = mm(u, wc_ref[...], NN)
    raw = mm(u, wd_ref[...], NT) + rows_ref[0:1]
    dt = jnp.maximum(raw, 0.0) + log1p_unit(jnp.exp(-jnp.abs(raw)))
    sig = 1.0 / (1.0 + jnp.exp(-raw))
    rate = -jnp.exp(rows_ref[1:2])
    cum = dot_right_full(triangle(length, True), dt * rate, NN)
    lane = iota(raw.shape, 1)
    tile = jnp.where(
        lane < heads,
        dt,
        jnp.where(lane < 2 * heads, pltpu.roll(cum, heads, 1), pltpu.roll(sig, 2 * heads, 1)),
    )
    half = heads // 2
    at = at_ref[0]
    mine = (LANES - half * at) % LANES
    for ref, shift in ((own_ref, mine), (snd_ref, (LANES - half * (1 - at)) % LANES)):
        ref[:, :state] = b
        ref[:, state : 2 * state] = c
        ref[:, 2 * state :] = pltpu.roll(tile, shift, 1)
    row = iota((8, LANES), 0)
    both = jnp.where(row == 0, jnp.broadcast_to(rate, (8, LANES)), rows_ref[...])
    misc_ref[...] = pltpu.roll(both, mine, 1)


def local_states(x, g, pack_ref, heads, width, start):
    half = heads // 2
    state = (pack_ref.shape[1] - LANES) // 2
    spread = expand_matrix(start, width, x.shape[1])
    dt, _, from_start, to_end, decay = coefficients(pack_ref[:, 2 * state :], heads, half)
    dt_wide = dot_left(dt, spread, NN)
    te_wide = dot_left(to_end, spread, NN)
    xw = x * (dt_wide * te_wide)
    gw = g * dot_left(from_start, spread, NN)
    s = dot3(pack_ref[:, :state], xw, TN)
    back = dot3(pack_ref[:, state : 2 * state], gw, TN)
    return s, back, dot_left_full(row_of(decay), spread, NN), dt_wide, te_wide, xw, gw


def intra_pairs(x_ref, g_ref, tile, scores, cumt_ref, acc_ref, rows_ref, back_ref, heads, width, pair0, pairs, unroll):
    length = scores.shape[0]
    src, dst = iota((length, length), 0), iota((length, length), 1)
    causal = dst >= src
    low = iota((length, LANES), 1) < width

    def step(k, _):
        at = pl.multiple_of(k * LANES, LANES)
        xp = x_ref[:, pl.ds(at, LANES)]
        gp = g_ref[:, pl.ds(at, LANES)]
        zero = jnp.zeros_like(xp)
        x2 = jnp.concatenate([jnp.where(low, xp, zero), jnp.where(low, zero, xp)], axis=0)
        g2 = jnp.concatenate([jnp.where(low, gp, zero), jnp.where(low, zero, gp)], axis=0)
        dots = mm(x2, gp, NT)
        turned = pltpu.roll(tile, LANES - 2 * (k + pair0), 1)
        his, los = [], []
        total = 0.0
        for e in range(2):
            h = 2 * (k + pair0) + e
            dt_col = jnp.broadcast_to(turned[:, e : e + 1], (length, length))
            cum_col = jnp.broadcast_to(turned[:, heads + e : heads + e + 1], (length, length))
            cum_row = cumt_ref[pl.ds(h, 1), :]
            table = jnp.exp(jnp.where(causal, cum_row - cum_col, -1e30))
            both = table * dots[e * length : (e + 1) * length] * dt_col
            total = total + both
            rows_ref[pl.ds(h, 1), :] = jnp.sum(both * scores, axis=0, keepdims=True)
            hi, lo = split2(table * scores)
            his.append(hi)
            los.append(lo)
        acc_ref[...] += total
        back_ref[:, pl.ds(at, LANES)] = mm_sum(
            [(jnp.concatenate(los, axis=1), g2), (jnp.concatenate(his, axis=1), g2)], NN
        )
        return 0

    lax.fori_loop(0, pairs, step, 0, unroll=unroll)


def own_kernel(
    xo_ref, go_ref, po_ref, back_ref, gbc_ref, rows_ref, s_ref, b_ref, d_ref, dt_ref, te_ref, xw_ref, gw_ref,
    cumt_ref, acc_ref, *, heads, width,
):
    state = (po_ref.shape[1] - LANES) // 2
    b = po_ref[:, :state]
    c = po_ref[:, state : 2 * state]
    tile = po_ref[:, 2 * state :]
    cumt_ref[...] = jnp.transpose(pltpu.roll(tile, LANES - heads, 1))
    acc_ref[...] = jnp.zeros_like(acc_ref)
    rows_ref[...] = jnp.zeros_like(rows_ref)
    intra_pairs(
        xo_ref, go_ref, tile, dot3(b, c, NT), cumt_ref, acc_ref, rows_ref, back_ref,
        heads, width, 0, xo_ref.shape[1] // LANES, 2,
    )
    acc = acc_ref[...]
    gbc_ref[:, :state] = dot3(acc, c, NN)
    gbc_ref[:, state:] = dot3(acc, b, TN)
    outs = local_states(xo_ref[...].astype(F32), go_ref[...].astype(F32), po_ref, heads, width, 0)
    for ref, value in zip((s_ref, b_ref, d_ref, dt_ref, te_ref, xw_ref, gw_ref), outs):
        ref[...] = value


def state_kernel(
    at_ref, xgr_ref, pr_ref, s_ref, b_ref, d_ref,
    even_ref, odd_ref, sf_ref, gs_ref, dp_ref, dr_ref, dt_ref, te_ref, xw_ref, gw_ref, *, heads, width, chunk,
):
    first_is_own = at_ref[0] == 0
    even = at_ref[1] == 0
    cols = lanes_of(chunk)
    s_own, b_own, d_own = s_ref[:, cols], b_ref[:, cols], d_ref[:, cols]
    s_rcv, b_rcv, d_rcv, *rest = local_states(xgr_ref[0], xgr_ref[1], pr_ref, heads, width, chunk[0] // width)

    def pick(a, b):
        return jnp.where(first_is_own, a, b)

    s_first, s_second = pick(s_own, s_rcv), pick(s_rcv, s_own)
    b_first, b_second = pick(b_own, b_rcv), pick(b_rcv, b_own)
    d_first, d_second = pick(d_own, d_rcv), pick(d_rcv, d_own)
    p = d_second[:1] * s_first + s_second
    q = d_first[:1] * b_second + b_first
    even_ref[...] = jnp.where(even, p, q)
    odd_ref[...] = jnp.where(even, q, p)
    sf_ref[...] = s_first
    gs_ref[...] = b_second
    dp_ref[...] = d_first * d_second
    dr_ref[...] = d_rcv
    for ref, value in zip((dt_ref, te_ref, xw_ref, gw_ref), rest):
        ref[...] = value


def intra_kernel(xgr_ref, pr_ref, *refs, heads, width, chunk, last):
    if chunk[0]:
        acc_in_ref, rows_in_ref, *refs = refs
    if last:
        back_ref, gbc_ref, rows_ref, x_ref, g_ref, cumt_ref, acc_ref = refs
    else:
        back_ref, acc_ref, rows_ref, x_ref, g_ref, cumt_ref = refs
    state = (pr_ref.shape[1] - LANES) // 2
    b = pr_ref[:, :state]
    c = pr_ref[:, state : 2 * state]
    tile = pr_ref[:, 2 * state :]
    x_ref[...] = xgr_ref[0].astype(BF16)
    g_ref[...] = xgr_ref[1].astype(BF16)
    cumt_ref[...] = jnp.transpose(pltpu.roll(tile, LANES - heads, 1))
    acc_ref[...] = acc_in_ref[...] if chunk[0] else jnp.zeros(acc_ref.shape, F32)
    rows_ref[...] = rows_in_ref[...] if chunk[0] else jnp.zeros(rows_ref.shape, F32)
    intra_pairs(
        x_ref, g_ref, tile, dot3(b, c, NT), cumt_ref, acc_ref, rows_ref, back_ref,
        heads, width, chunk[0] // LANES, chunk[1] // LANES, True,
    )
    if last:
        acc = acc_ref[...]
        gbc_ref[:, :state] = dot3(acc, c, NN)
        gbc_ref[:, state:] = dot3(acc, b, TN)


def carry_kernel(at_ref, *refs, heads, width, chunk, last):
    now_ref, before_ref, sf_ref, gs_ref, misc_ref, xo_ref, go_ref, xgr_ref, *refs = refs
    own_refs, rcv_refs, refs = refs[:7], refs[7:14], refs[14:]
    if chunk[0]:
        gbc_in_ref, sums_in_ref, small_in_ref, *refs = refs
    if last:
        gbc_own_ref, gbc_rcv_ref, rows_own_ref, rows_rcv_ref, *refs = refs
        gxo_ref, gxs_ref, pko_ref, pks_ref, extra_ref = refs
    else:
        gxo_ref, gxs_ref, gbc_ref, sums_ref, small_ref = refs
    half = heads // 2
    lanes = chunk[1]
    cols = lanes_of(chunk)
    own_first = at_ref[0] == 0
    even = at_ref[1] == 0
    packs = (own_refs[0], rcv_refs[0])
    length = packs[0].shape[0]
    state = (packs[0].shape[1] - LANES) // 2
    spread = expand_matrix(chunk[0] // width, width, lanes)
    collect = collect_matrix(chunk[0] // width, width, lanes)
    skip_row = jnp.where(iota((1, LANES), 1) < half, misc_ref[2:3], 0.0)
    skip_wide = dot_left_full(row_of(skip_row), spread, NN)[:1]
    decays = (own_refs[2][:1, cols], rcv_refs[2][:1])
    now, before = now_ref[...], before_ref[...]
    cin, cout = jnp.where(even, before, now), jnp.where(even, now, before)
    d_first = jnp.where(own_first, decays[0], decays[1])
    d_second = jnp.where(own_first, decays[1], decays[0])
    cin_second = d_first * cin + sf_ref[...]
    cout_first = d_second * cout + gs_ref[...]
    gb, gc, sums, ends, skips = [], [], [], [], 0.0
    for w in (0, 1):
        is_first = own_first if w == 0 else jnp.logical_not(own_first)
        my_in = jnp.where(is_first, cin, cin_second)
        my_out = jnp.where(is_first, cout_first, cout)
        if w == 0:
            x, g = xo_ref[:, cols].astype(F32), go_ref[:, cols].astype(F32)
            intra, dt_wide, te_wide, xw, gw = [own_refs[i][:, cols] for i in (1, 3, 4, 5, 6)]
        else:
            x, g = xgr_ref[0], xgr_ref[1]
            intra, dt_wide, te_wide, xw, gw = [rcv_refs[i][...] for i in (1, 3, 4, 5, 6)]
        b, c = packs[w][:, :state], packs[w][:, state : 2 * state]
        front = dot3(c, my_in, NN)
        back = dot3(b, my_out, NN)
        back_in = intra + te_wide * back
        grad_x = dt_wide * back_in + skip_wide * g
        if w == 0:
            gxo_ref[...] = grad_x.astype(BF16)
        else:
            gxs_ref[...] = grad_x
        sums.append([dot_left_full(v, collect, NN) for v in (x * back_in, gw * front)])
        gb.append(dot3(xw, my_out, NT))
        gc.append(dot3(gw, my_in, NT))
        ends.append(decays[w] * jnp.sum(my_in * my_out, axis=0, keepdims=True) + jnp.sum(xw * back, axis=0, keepdims=True))
        skips = skips + jnp.sum(x * g, axis=0, keepdims=True)
    row = iota((8, lanes), 0)
    stacked = jnp.where(row == 0, ends[0], jnp.where(row == 1, ends[1], jnp.where(row == 2, skips, 0.0)))
    small = dot_left_full(stacked, collect, NN)
    if chunk[0]:
        gb = [gb[w] + gbc_in_ref[w, :, :state] for w in (0, 1)]
        gc = [gc[w] + gbc_in_ref[w, :, state:] for w in (0, 1)]
        sums = [[sums[w][i] + sums_in_ref[w, i] for i in range(2)] for w in (0, 1)]
        small = small + small_in_ref[...]
    if not last:
        for w in (0, 1):
            gbc_ref[w, :, :state] = gb[w]
            gbc_ref[w, :, state:] = gc[w]
            for i in range(2):
                sums_ref[w, i] = sums[w][i]
        small_ref[...] = small
        return
    rate = misc_ref[0:1]
    later = triangle(length, False)
    last_row = iota((length, LANES), 0) == length - 1
    bias_sum = jnp.zeros((1, LANES), F32)
    alog_sum = jnp.zeros((1, LANES), F32)
    lane = iota((length, LANES), 1) < half
    for w, out_ref in ((0, pko_ref), (1, pks_ref)):
        tile = packs[w][:, 2 * state :]
        dt = jnp.where(lane, tile, 0.0)
        sig = pltpu.roll(tile, LANES - 2 * heads, 1)
        direct, ahead = sums[w]
        intra_rows = (rows_own_ref, rows_rcv_ref)[w]
        change = jnp.transpose(intra_rows[...]) + ahead - dt * direct
        change = change + jnp.where(last_row, small[w : w + 1], 0.0)
        grad_log = dot_right_full(later, change, NN)
        grad_raw = jnp.where(lane, (direct + grad_log * rate) * sig, 0.0)
        bias_sum = bias_sum + jnp.sum(grad_raw, axis=0, keepdims=True)
        alog_sum = alog_sum + jnp.sum(grad_log * dt, axis=0, keepdims=True) * rate
        intra_gbc = (gbc_own_ref, gbc_rcv_ref)[w]
        out_ref[:, :state] = gb[w] + intra_gbc[:, :state]
        out_ref[:, state : 2 * state] = gc[w] + intra_gbc[:, state:]
        out_ref[:, 2 * state :] = grad_raw
    row = iota((8, LANES), 0)
    extra = jnp.where(row == 0, bias_sum, jnp.where(row == 1, alog_sum, jnp.where(row == 2, small[2:3], 0.0)))
    extra_ref[...] = jnp.where(iota((8, LANES), 1) < half, extra, 0.0)


def join_kernel(at_ref, own_ref, rcv_ref, extra_ref, out_ref, extra_out_ref, *, heads):
    state = (own_ref.shape[1] - LANES) // 2
    half = heads // 2
    at = at_ref[0]
    out_ref[0, :, : 2 * state] = own_ref[:, : 2 * state] + rcv_ref[:, : 2 * state]
    mine = pltpu.roll(own_ref[:, 2 * state :], half * at, 1)
    other = pltpu.roll(rcv_ref[:, 2 * state :], half * (1 - at), 1)
    out_ref[0, :, 2 * state :] = mine + other
    extra_out_ref[...] = pltpu.roll(extra_ref[...], half * at, 1)


def merge_kernel(at_ref, *refs, chunks):
    out_ref = refs[-1]
    half_lanes = out_ref.shape[1] // 2
    for i, (start, lanes) in enumerate(chunks):
        mine = pl.multiple_of(at_ref[0] * half_lanes + start, LANES)
        other = pl.multiple_of((1 - at_ref[0]) * half_lanes + start, LANES)
        out_ref[:, pl.ds(mine, lanes)] = refs[i][...]
        out_ref[:, pl.ds(other, lanes)] = refs[len(chunks) + i][...].astype(BF16)


def grad_u_kernel(cols_ref, wb_ref, wc_ref, wd_ref, out_ref):
    state = wb_ref.shape[1]
    cols = cols_ref[0]
    total = dot_left(cols[:, :state], wb_ref[...], NT)
    total = total + dot_left(cols[:, state : 2 * state], wc_ref[...], NT)
    total = total + dot_left(cols[:, 2 * state :], wd_ref[...], NN)
    out_ref[...] = total.astype(BF16)


def weight_kernel(*refs, pieces, heads, state):
    u = jnp.concatenate([r[i].astype(BF16) for r in refs[:pieces] for i in range(r.shape[0])], axis=0)
    cols = jnp.concatenate([r[i] for r in refs[pieces:-2] for i in range(r.shape[0])], axis=0)
    extra_ref, out_ref = refs[-2:]
    count, block, _ = out_ref.shape
    each = (block - heads) // 2
    hi, lo = split2(cols[:, : 2 * state])
    wide = mm(u, hi, TN) + mm(u, lo, TN)
    thi, tlo = split2(cols[:, 2 * state :])
    turned = mm(thi, u, TN) + mm(tlo, u, TN)
    turned = jnp.concatenate([turned[:heads], jnp.zeros((heads, LANES), F32)], axis=1)
    tail = jnp.transpose(jnp.concatenate([extra_ref[...], jnp.zeros((LANES - 8, LANES), F32)], axis=0))
    tail = pltpu.roll(tail, each, 1)[:heads]
    lane = iota((heads, LANES), 1)
    for s in range(count):
        rows = slice(s * each, (s + 1) * each)
        out_ref[s, :each] = wide[rows, :state]
        out_ref[s, each : 2 * each] = wide[rows, state:]
        start = s * each // LANES * LANES
        window = pltpu.roll(turned[:, start : start + 2 * LANES], (2 * LANES + start - s * each) % (2 * LANES), 1)
        out_ref[s, 2 * each :] = jnp.where(lane < each, window[:, :LANES], tail)


def final_kernel(at_ref, *refs, pieces, heads, order):
    parts = [r[i] for r in refs[:pieces] for i in range(r.shape[0])]
    gb_ref, gc_ref, gd_ref, bias_ref, alog_ref, skip_ref = refs[pieces:]
    rows_out = gb_ref.shape[0]
    each = rows_out // len(parts)
    mine = at_ref[2]
    total, wide = 0.0, 0.0
    around = -(-rows_out // LANES) * LANES + LANES
    for d in range(len(parts)):
        block = parts[0]
        for part, flip in list(zip(parts, order))[1:]:
            block = jnp.where(mine == d ^ flip, part, block)
        rows = slice(d * each, (d + 1) * each)
        gb_ref[rows] = block[:each]
        gc_ref[rows] = block[each : 2 * each]
        tail = block[2 * each :]
        total = total + tail
        tail = jnp.where(iota(tail.shape, 1) < each, tail, 0.0)
        tail = jnp.concatenate([tail, jnp.zeros((heads, around - LANES), F32)], axis=1)
        wide = wide + (pltpu.roll(tail, d * each, 1) if d else tail)
    gd_ref[...] = wide[:, :rows_out]
    total = jnp.concatenate([total, jnp.zeros((LANES - heads, LANES), F32)], axis=0)
    turned = jnp.transpose(total)
    bias_ref[...] = turned[each : each + 1, :heads]
    alog_ref[...] = turned[each + 1 : each + 2, :heads]
    skip_ref[...] = turned[each + 2 : each + 3, :heads]


def vmem(n):
    return [pl.BlockSpec(memory_space=pltpu.VMEM) for _ in range(n)]


def call(kernel, args, outs, scratch=(), scalars=None, flops=10**8, stay=False):
    specs = [pl.BlockSpec(memory_space=pltpu.HBM) for _ in args] if stay else vmem(len(args))
    if scalars is not None:
        specs, args = [pl.BlockSpec(memory_space=pltpu.SMEM)] + specs, [scalars, *args]
    return pl.pallas_call(
        kernel,
        in_specs=specs,
        out_specs=vmem(len(outs)),
        out_shape=[jax.ShapeDtypeStruct(s, t) for s, t in outs],
        scratch_shapes=list(scratch),
        cost_estimate=pl.CostEstimate(flops=flops, transcendentals=0, bytes_accessed=10**6),
        compiler_params=pltpu.CompilerParams(vmem_limit_bytes=12 << 20),
    )(*args)


def chunk_list(half, width):
    pairs = half * width // LANES
    whole = sum(SHARES)
    ends = [round(pairs * sum(SHARES[: i + 1]) / whole) for i in range(len(SHARES))]
    starts = [0] + ends[:-1]
    return [(a * LANES, (b - a) * LANES) for a, b in zip(starts, ends) if b > a]


def body(layer_input, ssm_input, out_grad, b_weight, c_weight, dt_weight, dt_bias, a_log, d_skip):
    length, model = layer_input.shape
    heads = dt_bias.shape[0]
    state = b_weight.shape[1]
    width = ssm_input.shape[1] // heads
    half = heads // 2
    lanes = half * width
    chunks = chunk_list(half, width)
    final = len(chunks) - 1
    count = lax.axis_size("seq")
    where = lax.axis_index("seq")
    place = where % 2
    level = where // 2
    levels = count // 2
    groups = lax.axis_size("dp")
    group = lax.axis_index("dp")
    each = model // count // groups
    bits = []
    while groups >> (len(bits) + 1):
        bits.insert(0, 1 << len(bits))
    at = lax.optimization_barrier(jnp.stack([place, level % 2, group]).astype(jnp.int32))
    swap = [(i, i ^ 1) for i in range(count)]
    rounds = []
    for r in range(levels - 1):
        pairs = []
        for z in range(r % 2, levels - 1, 2):
            for i in range(2):
                a, b = 2 * z + i, 2 * z + 2 + i
                pairs += [(a, b), (b, a)]
        rounds.append(pairs)
    pack = 2 * state + LANES

    def exchange(value):
        return lax.ppermute(value, "seq", swap)

    def spread_pieces(value):
        pieces = [value]
        for bit in bits:
            pairs = [(d, d ^ bit) for d in range(groups)]
            for piece in list(pieces):
                pieces.append(lax.ppermute(piece, "dp", pairs))
        return pieces

    def swap_columns(sent, bit):
        return lax.ppermute(sent, "dp", [(d, d ^ bit) for d in range(groups)])

    def column_pieces(value):
        left = list(bits)
        if each % 16 == 0 and groups > 1:
            shape = (groups // 2, 1, length, count * each)
            keep, sent = call(
                functools.partial(columns_kernel, count=count, groups=groups, each=each),
                [value], [(shape, BF16), (shape, F32)], scalars=at,
            )
            pieces = [keep, swap_columns(sent, left.pop(0))]
        else:
            value = value.reshape(length, count, groups, each).transpose(2, 0, 1, 3)
            pieces = [value.reshape(groups, 1, length, count * each)]
        for bit in left:
            shape = (bit, sum(p.shape[1] for p in pieces), length, count * each)
            keep, sent = call(
                functools.partial(halve_kernel, bit=bit), pieces,
                [(shape, BF16), (shape, F32)], scalars=at,
            )
            pieces = [keep, swap_columns(sent, bit)]
        return [p[0] for p in pieces]

    (sent,) = call(
        functools.partial(send_kernel, half_lanes=lanes, start=0), [ssm_input, out_grad],
        [((2, length, chunks[0][1]), F32)], scalars=at, stay=True,
        scratch=[pltpu.VMEM((2, length, chunks[0][1]), BF16), pltpu.SemaphoreType.DMA((2,))],
    )
    received = [exchange(sent)]
    wd = jnp.pad(dt_weight.T, ((0, LANES - heads), (0, 0)))
    rows = jnp.pad(jnp.stack([dt_bias, a_log, d_skip]), ((0, 5), (0, LANES - heads)))
    own, send, misc = call(
        functools.partial(proj_kernel, heads=heads),
        [layer_input, b_weight, c_weight, wd, rows],
        [((length, pack), F32)] * 2 + [((8, LANES), F32)], scalars=at,
    )
    rcv = exchange(send)
    x_own, g_own, *sent = call(
        functools.partial(keep_kernel, half_lanes=lanes, chunks=chunks[1:]), [ssm_input, out_grad],
        [((length, lanes), BF16)] * 2 + [((2, length, c[1]), F32) for c in chunks[1:]], scalars=at, stay=True,
        scratch=[
            pltpu.VMEM((2, length, max(lanes - chunks[0][1], LANES)), BF16),
            pltpu.SemaphoreType.DMA((2,)),
            pltpu.SemaphoreType.DMA((2,)),
        ],
    )
    send, *sent = lax.optimization_barrier((send, *sent))
    received += [exchange(v) for v in sent]
    u_pieces = column_pieces(layer_input)

    full = ((length, lanes), F32)
    back_own, gbc_own, rows_own, s_own, b_own, *own_rest = call(
        functools.partial(own_kernel, heads=heads, width=width), [x_own, g_own, own],
        [full, ((length, 2 * state), F32), ((LANES, length), F32), ((state, lanes), F32), ((state, lanes), F32)]
        + [((8, lanes), F32)] + [full] * 4,
        scratch=[pltpu.VMEM((LANES, length), F32), pltpu.VMEM((length, length), F32)], flops=10**9,
    )
    mine_all = [own, back_own, *own_rest]
    acc = rows_sum = None
    sums = []
    gx_own, gx_rcv = [], []
    for j, chunk in enumerate(chunks):
        last = j == final
        wide, tall = ((state, chunk[1]), F32), ((length, chunk[1]), F32)
        even, odd, s_first, g_second, decay, *rest = call(
            functools.partial(state_kernel, heads=heads, width=width, chunk=chunk),
            [received[j], rcv, s_own, b_own, own_rest[0]],
            [wide] * 4 + [((8, chunk[1]), F32)] * 2 + [tall] * 4, scalars=at,
        )
        decay = decay[:1]
        now = before = jnp.zeros((state, chunk[1]), F32)
        for r, pairs in enumerate(rounds):
            value = (even, odd)[r % 2]
            if r:
                value = value + decay * now
            before = now
            now = lax.ppermute(value, "seq", pairs)
        back, acc, rows_sum = call(
            functools.partial(intra_kernel, heads=heads, width=width, chunk=chunk, last=last),
            [received[j], rcv] + ([acc, rows_sum] if j else []),
            [tall, ((length, 2 * state if last else length), F32), ((LANES, length), F32)],
            scratch=[pltpu.VMEM((length, chunk[1]), BF16)] * 2 + [pltpu.VMEM((LANES, length), F32)]
            + ([pltpu.VMEM((length, length), F32)] if last else []),
            flops=10**9,
        )
        outs = [((length, chunk[1]), BF16), tall]
        if last:
            outs += [((length, pack), F32)] * 2 + [((8, LANES), F32)]
        else:
            outs += [((2, length, 2 * state), F32), ((2, 2, length, LANES), F32), ((8, LANES), F32)]
        mine, theirs, *sums = call(
            functools.partial(carry_kernel, heads=heads, width=width, chunk=chunk, last=last),
            [now, before, s_first, g_second, misc, x_own, g_own, received[j]]
            + mine_all + [rcv, back, *rest] + sums
            + ([gbc_own, acc, rows_own, rows_sum] if last else []),
            outs, scalars=at,
        )
        gx_own.append(mine)
        if last:
            pack_own, pack_send, extra = sums
            pack_rcv = exchange(pack_send)
        gx_rcv.append(exchange(theirs))
    cols, extra = call(
        functools.partial(join_kernel, heads=heads), [pack_own, pack_rcv, extra],
        [((1, length, pack), F32), ((8, LANES), F32)], scalars=at,
    )
    gathered = spread_pieces(cols)
    (grad_u,) = call(grad_u_kernel, [cols, b_weight, c_weight, wd], [((length, model), BF16)])
    (grad_x,) = call(
        functools.partial(merge_kernel, chunks=chunks), [*gx_own, *gx_rcv],
        [((length, 2 * lanes), BF16)], scalars=at,
    )
    (blocks,) = call(
        functools.partial(weight_kernel, pieces=len(u_pieces), heads=heads, state=state),
        [*u_pieces, *gathered, extra], [((count, 2 * each + heads, LANES), F32)],
    )
    moved = lax.all_to_all(blocks, "seq", 0, 0, tiled=True)
    (moved,) = call(total_kernel, [moved], [((1, 2 * each + heads, LANES), F32)])
    parts = spread_pieces(moved)
    order = [0]
    for bit in bits:
        order = order + [f ^ bit for f in order]
    rows_out = model // count
    gb, gc, gd, bias, alog, skip = call(
        functools.partial(final_kernel, pieces=len(parts), heads=heads, order=order), parts,
        [((rows_out, state), F32)] * 2 + [((heads, rows_out), F32)] + [((1, heads), F32)] * 3, scalars=at,
    )
    return grad_x, grad_u, gb, gc, gd.T, bias[0], alog[0], skip[0]


def solution(mesh):
    rows = P(("dp", "seq"), None)
    in_specs = (rows, rows, rows, P(), P(), P(), P(), P(), P())
    out_specs = (rows, rows, P("seq", None), P("seq", None), P("seq", None), P(), P(), P())
    return jax.shard_map(body, mesh=mesh, in_specs=in_specs, out_specs=out_specs, check_vma=False)
```

```python
import functools

import jax
import jax.numpy as jnp
from jax import lax
from jax.experimental import pallas as pl
from jax.experimental.pallas import tpu as pltpu
from jax.sharding import PartitionSpec as P


F32 = jnp.float32
BF16 = jnp.bfloat16
LANES = 128
SHARES = (8, 8, 4)

NN = (((1,), (0,)), ((), ()))
NT = (((1,), (1,)), ((), ()))
TN = (((0,), (0,)), ((), ()))


def mm(a, b, dims):
    return lax.dot_general(a, b, dims, preferred_element_type=F32)


def split2(a):
    hi = a.astype(BF16)
    return hi, (a - hi.astype(F32)).astype(BF16)


def split3(a):
    hi = a.astype(BF16)
    rest = a - hi.astype(F32)
    mid = rest.astype(BF16)
    return hi, mid, (rest - mid.astype(F32)).astype(BF16)


def mm_sum(terms, dims):
    (left,), (right,) = dims[0]
    a = jnp.concatenate([t[0] for t in terms], axis=left)
    b = jnp.concatenate([t[1] for t in terms], axis=right)
    return mm(a, b, dims)


def dot3(a, b, dims):
    ah, al = split2(a)
    bh, bl = split2(b)
    return mm_sum([(al, bh), (ah, bl), (ah, bh)], dims)


def dot_left(a, b, dims):
    ah, al = split2(a)
    return mm_sum([(al, b), (ah, b)], dims)


def dot_left_full(a, b, dims):
    ah, am, al = split3(a)
    return mm_sum([(al, b), (am, b), (ah, b)], dims)


def dot_right_full(a, b, dims):
    bh, bm, bl = split3(b)
    return mm_sum([(a, bl), (a, bm), (a, bh)], dims)


def iota(shape, axis):
    return lax.broadcasted_iota(jnp.int32, shape, axis)


def log1p_unit(y):
    s = y / (2.0 + y)
    q = s * s
    poly = jnp.full_like(q, 1.0 / 17)
    for k in (15, 13, 11, 9, 7, 5, 3, 1):
        poly = poly * q + 1.0 / k
    return 2.0 * s * poly


def triangle(length, lower):
    r, c = iota((length, length), 0), iota((length, length), 1)
    keep = (r >= c) if lower else (c >= r)
    return jnp.where(keep, 1.0, 0.0).astype(BF16)


def expand_matrix(head_start, width, lanes):
    r, c = iota((LANES, lanes), 0), iota((LANES, lanes), 1)
    return jnp.where(r == head_start + c // width, 1.0, 0.0).astype(BF16)


def collect_matrix(head_start, width, lanes):
    r, c = iota((lanes, LANES), 0), iota((lanes, LANES), 1)
    return jnp.where(c == head_start + r // width, 1.0, 0.0).astype(BF16)


def coefficients(tile, heads_all, heads_half):
    lane = iota(tile.shape, 1) < heads_half
    length = tile.shape[0]
    dt = jnp.where(lane, tile, 0.0)
    cum = jnp.where(lane, pltpu.roll(tile, LANES - heads_all, 1), 0.0)
    last = cum[length - 1 : length, :]
    from_start = jnp.where(lane, jnp.exp(cum), 0.0)
    to_end = jnp.where(lane, jnp.exp(last - cum), 0.0)
    decay = jnp.where(lane[:1], jnp.exp(last), 0.0)
    return dt, cum, from_start, to_end, decay


def row_of(v, rows=8):
    return jnp.broadcast_to(v, (rows, v.shape[1]))


def lanes_of(chunk):
    return slice(chunk[0], chunk[0] + chunk[1])


def send_kernel(at_ref, x_ref, g_ref, out_ref, buf_ref, sems, *, half_lanes, start):
    part = out_ref.shape[2]
    first = pl.multiple_of((1 - at_ref[0]) * half_lanes + start, LANES)
    copies = []
    for i, ref in enumerate((x_ref, g_ref)):
        copies.append(pltpu.make_async_copy(ref.at[:, pl.ds(first, part)], buf_ref.at[i], sems.at[i]))
        copies[-1].start()
    for i, copy in enumerate(copies):
        copy.wait()
        out_ref[i] = buf_ref[i].astype(F32)


def keep_kernel(at_ref, x_ref, g_ref, *refs, half_lanes, chunks):
    keeps, sends = refs[:2], refs[2 : 2 + len(chunks)]
    buf_ref, keep_sems, send_sems = refs[2 + len(chunks) :]
    own = pl.multiple_of(at_ref[0] * half_lanes, LANES)
    other = pl.multiple_of((1 - at_ref[0]) * half_lanes, LANES)
    rest = half_lanes - chunks[0][0] if chunks else 0
    sending, keeping = [], []
    for i, ref in enumerate((x_ref, g_ref)):
        if chunks:
            source = ref.at[:, pl.ds(pl.multiple_of(other + chunks[0][0], LANES), rest)]
            sending.append(pltpu.make_async_copy(source, buf_ref.at[i], send_sems.at[i]))
            sending[-1].start()
        keeping.append(pltpu.make_async_copy(ref.at[:, pl.ds(own, half_lanes)], keeps[i], keep_sems.at[i]))
        keeping[-1].start()
    for i, copy in enumerate(sending):
        copy.wait()
        for chunk, out_ref in zip(chunks, sends):
            first = chunk[0] - chunks[0][0]
            out_ref[i] = buf_ref[i, :, first : first + chunk[1]].astype(F32)
    for copy in keeping:
        copy.wait()


def columns_kernel(at_ref, u_ref, keep_ref, send_ref, *, levels, groups, each):
    u = u_ref[...].astype(F32)
    taken = []
    for d in range(groups):
        for p in range(2):
            starts = [((2 * z + p) * groups + d) * each for z in range(levels)]
            parts = [u[:, a : a + each] for a in starts]
            room = keep_ref.shape[3] - levels * each
            taken.append(jnp.concatenate(parts + [jnp.zeros((u.shape[0], room), F32)] * (room > 0), axis=1))
    half = groups
    high = at_ref[2] >= groups // 2
    for i in range(half):
        keep_ref[i, 0] = jnp.where(high, taken[half + i], taken[i]).astype(BF16)
        send_ref[i, 0] = jnp.where(high, taken[i], taken[half + i])


def halve_kernel(at_ref, *refs, which, bit):
    keep_ref, send_ref = refs[-2:]
    high = (at_ref[which] // bit) % 2 == 1
    half = keep_ref.shape[0]
    done = 0
    for ref in refs[:-2]:
        for k in range(ref.shape[1]):
            for i in range(half):
                low_part, high_part = ref[i, k].astype(F32), ref[half + i, k].astype(F32)
                keep_ref[i, done + k] = jnp.where(high, high_part, low_part).astype(BF16)
                send_ref[i, done + k] = jnp.where(high, low_part, high_part)
        done += ref.shape[1]


def total_kernel(*refs):
    total = refs[0][...]
    for ref in refs[1:-1]:
        total = total + ref[...]
    refs[-1][...] = total


FOLD = 32


def folded(tile):
    rows = tile.shape[0] // (LANES // FOLD)
    lane = iota((rows, LANES), 1) // FOLD
    out = tile[:rows]
    for q in range(1, LANES // FOLD):
        out = jnp.where(lane == q, pltpu.roll(tile[q * rows : (q + 1) * rows], q * FOLD, 1), out)
    return out


def unfolded(tile):
    parts = [tile] + [pltpu.roll(tile, LANES - q * FOLD, 1) for q in range(1, LANES // FOLD)]
    out = jnp.concatenate(parts, axis=0)
    return jnp.where(iota(out.shape, 1) < FOLD, out, 0.0)


def proj_kernel(at_ref, u_ref, wb_ref, wc_ref, wd_ref, rows_ref, own_ref, snd_ref, misc_ref, *, heads):
    length = u_ref.shape[0]
    state = wb_ref.shape[1]
    u = u_ref[...]
    b = mm(u, wb_ref[...], NN)
    c = mm(u, wc_ref[...], NN)
    raw = mm(u, wd_ref[...], NT) + rows_ref[0:1]
    dt = jnp.maximum(raw, 0.0) + log1p_unit(jnp.exp(-jnp.abs(raw)))
    sig = 1.0 / (1.0 + jnp.exp(-raw))
    rate = -jnp.exp(rows_ref[1:2])
    cum = dot_right_full(triangle(length, True), dt * rate, NN)
    lane = iota(raw.shape, 1)
    tile = jnp.where(
        lane < heads,
        dt,
        jnp.where(lane < 2 * heads, pltpu.roll(cum, heads, 1), pltpu.roll(sig, 2 * heads, 1)),
    )
    half = heads // 2
    at = at_ref[0]
    mine = (LANES - half * at) % LANES
    for ref, shift in ((own_ref, mine), (snd_ref, (LANES - half * (1 - at)) % LANES)):
        ref[:, :state] = b
        ref[:, state : 2 * state] = c
        ref[:, 2 * state :] = pltpu.roll(tile, shift, 1)
    row = iota((8, LANES), 0)
    both = jnp.where(row == 0, jnp.broadcast_to(rate, (8, LANES)), rows_ref[...])
    misc_ref[...] = pltpu.roll(both, mine, 1)


def local_states(x, g, pack_ref, heads, width, start):
    half = heads // 2
    state = (pack_ref.shape[1] - LANES) // 2
    spread = expand_matrix(start, width, x.shape[1])
    dt, _, from_start, to_end, decay = coefficients(pack_ref[:, 2 * state :], heads, half)
    dt_wide = dot_left(dt, spread, NN)
    te_wide = dot_left(to_end, spread, NN)
    xw = x * (dt_wide * te_wide)
    gw = g * dot_left(from_start, spread, NN)
    s = dot3(pack_ref[:, :state], xw, TN)
    back = dot3(pack_ref[:, state : 2 * state], gw, TN)
    return s, back, dot_left_full(row_of(decay), spread, NN), dt_wide, te_wide, xw, gw


def intra_pairs(x_ref, g_ref, tile, scores, cumt_ref, acc_ref, rows_ref, back_ref, heads, width, pair0, pairs, unroll):
    length = scores.shape[0]
    src, dst = iota((length, length), 0), iota((length, length), 1)
    causal = dst >= src
    low = iota((length, LANES), 1) < width

    def step(k, _):
        at = pl.multiple_of(k * LANES, LANES)
        xp = x_ref[:, pl.ds(at, LANES)]
        gp = g_ref[:, pl.ds(at, LANES)]
        zero = jnp.zeros_like(xp)
        x2 = jnp.concatenate([jnp.where(low, xp, zero), jnp.where(low, zero, xp)], axis=0)
        g2 = jnp.concatenate([jnp.where(low, gp, zero), jnp.where(low, zero, gp)], axis=0)
        dots = mm(x2, gp, NT)
        turned = pltpu.roll(tile, LANES - 2 * (k + pair0), 1)
        his, los = [], []
        total = 0.0
        for e in range(2):
            h = 2 * (k + pair0) + e
            dt_col = jnp.broadcast_to(turned[:, e : e + 1], (length, length))
            cum_col = jnp.broadcast_to(turned[:, heads + e : heads + e + 1], (length, length))
            cum_row = cumt_ref[pl.ds(h, 1), :]
            table = jnp.exp(jnp.where(causal, cum_row - cum_col, -1e30))
            both = table * dots[e * length : (e + 1) * length] * dt_col
            total = total + both
            rows_ref[pl.ds(h, 1), :] = jnp.sum(both * scores, axis=0, keepdims=True)
            hi, lo = split2(table * scores)
            his.append(hi)
            los.append(lo)
        acc_ref[...] += total
        back_ref[:, pl.ds(at, LANES)] = mm_sum(
            [(jnp.concatenate(los, axis=1), g2), (jnp.concatenate(his, axis=1), g2)], NN
        )
        return 0

    lax.fori_loop(0, pairs, step, 0, unroll=unroll)


def own_kernel(
    xo_ref, go_ref, po_ref, back_ref, gbc_ref, rows_ref, s_ref, b_ref, d_ref, dt_ref, te_ref, xw_ref, gw_ref,
    cumt_ref, acc_ref, *, heads, width,
):
    state = (po_ref.shape[1] - LANES) // 2
    b = po_ref[:, :state]
    c = po_ref[:, state : 2 * state]
    tile = po_ref[:, 2 * state :]
    cumt_ref[...] = jnp.transpose(pltpu.roll(tile, LANES - heads, 1))
    acc_ref[...] = jnp.zeros_like(acc_ref)
    rows_ref[...] = jnp.zeros_like(rows_ref)
    intra_pairs(
        xo_ref, go_ref, tile, dot3(b, c, NT), cumt_ref, acc_ref, rows_ref, back_ref,
        heads, width, 0, xo_ref.shape[1] // LANES, 2,
    )
    acc = acc_ref[...]
    gbc_ref[:, :state] = dot3(acc, c, NN)
    gbc_ref[:, state:] = dot3(acc, b, TN)
    outs = local_states(xo_ref[...].astype(F32), go_ref[...].astype(F32), po_ref, heads, width, 0)
    for ref, value in zip((s_ref, b_ref, d_ref, dt_ref, te_ref, xw_ref, gw_ref), outs):
        ref[...] = value


def state_kernel(
    at_ref, xgr_ref, pr_ref, s_ref, b_ref, d_ref,
    even_ref, odd_ref, sf_ref, gs_ref, dp_ref, dr_ref, dt_ref, te_ref, xw_ref, gw_ref, *, heads, width, chunk,
):
    first_is_own = at_ref[0] == 0
    even = at_ref[1] == 0
    cols = lanes_of(chunk)
    s_own, b_own, d_own = s_ref[:, cols], b_ref[:, cols], d_ref[:, cols]
    s_rcv, b_rcv, d_rcv, *rest = local_states(xgr_ref[0], xgr_ref[1], pr_ref, heads, width, chunk[0] // width)

    def pick(a, b):
        return jnp.where(first_is_own, a, b)

    s_first, s_second = pick(s_own, s_rcv), pick(s_rcv, s_own)
    b_first, b_second = pick(b_own, b_rcv), pick(b_rcv, b_own)
    d_first, d_second = pick(d_own, d_rcv), pick(d_rcv, d_own)
    p = d_second[:1] * s_first + s_second
    q = d_first[:1] * b_second + b_first
    even_ref[...] = jnp.where(even, p, q)
    odd_ref[...] = jnp.where(even, q, p)
    sf_ref[...] = s_first
    gs_ref[...] = b_second
    dp_ref[...] = d_first * d_second
    dr_ref[...] = d_rcv
    for ref, value in zip((dt_ref, te_ref, xw_ref, gw_ref), rest):
        ref[...] = value


def intra_kernel(xgr_ref, pr_ref, *refs, heads, width, chunk, last):
    if chunk[0]:
        acc_in_ref, rows_in_ref, *refs = refs
    if last:
        back_ref, gbc_ref, rows_ref, x_ref, g_ref, cumt_ref, acc_ref = refs
    else:
        back_ref, acc_ref, rows_ref, x_ref, g_ref, cumt_ref = refs
    state = (pr_ref.shape[1] - LANES) // 2
    b = pr_ref[:, :state]
    c = pr_ref[:, state : 2 * state]
    tile = pr_ref[:, 2 * state :]
    x_ref[...] = xgr_ref[0].astype(BF16)
    g_ref[...] = xgr_ref[1].astype(BF16)
    cumt_ref[...] = jnp.transpose(pltpu.roll(tile, LANES - heads, 1))
    acc_ref[...] = acc_in_ref[...] if chunk[0] else jnp.zeros(acc_ref.shape, F32)
    rows_ref[...] = rows_in_ref[...] if chunk[0] else jnp.zeros(rows_ref.shape, F32)
    intra_pairs(
        x_ref, g_ref, tile, dot3(b, c, NT), cumt_ref, acc_ref, rows_ref, back_ref,
        heads, width, chunk[0] // LANES, chunk[1] // LANES, True,
    )
    if last:
        acc = acc_ref[...]
        gbc_ref[:, :state] = dot3(acc, c, NN)
        gbc_ref[:, state:] = dot3(acc, b, TN)


def carry_kernel(at_ref, *refs, heads, width, chunk, last, came):
    now = sum(ref[...] for ref in refs[: came[0]])
    before = sum(ref[...] for ref in refs[came[0] : sum(came)])
    refs = refs[sum(came) :]
    sf_ref, gs_ref, misc_ref, xo_ref, go_ref, xgr_ref, *refs = refs
    own_refs, rcv_refs, refs = refs[:7], refs[7:14], refs[14:]
    if chunk[0]:
        gbc_in_ref, sums_in_ref, small_in_ref, *refs = refs
    if last:
        gbc_own_ref, gbc_rcv_ref, rows_own_ref, rows_rcv_ref, *refs = refs
        gxo_ref, gxs_ref, pk_ref = refs
    else:
        gxo_ref, gxs_ref, gbc_ref, sums_ref, small_ref = refs
    half = heads // 2
    lanes = chunk[1]
    cols = lanes_of(chunk)
    own_first = at_ref[0] == 0
    even = at_ref[1] == 0
    packs = (own_refs[0], rcv_refs[0])
    length = packs[0].shape[0]
    state = (packs[0].shape[1] - LANES) // 2
    spread = expand_matrix(chunk[0] // width, width, lanes)
    collect = collect_matrix(chunk[0] // width, width, lanes)
    skip_row = jnp.where(iota((1, LANES), 1) < half, misc_ref[2:3], 0.0)
    skip_wide = dot_left_full(row_of(skip_row), spread, NN)[:1]
    decays = (own_refs[2][:1, cols], rcv_refs[2][:1])
    cin, cout = jnp.where(even, before, now), jnp.where(even, now, before)
    d_first = jnp.where(own_first, decays[0], decays[1])
    d_second = jnp.where(own_first, decays[1], decays[0])
    cin_second = d_first * cin + sf_ref[...]
    cout_first = d_second * cout + gs_ref[...]
    gb, gc, sums, ends, skips = [], [], [], [], 0.0
    for w in (0, 1):
        is_first = own_first if w == 0 else jnp.logical_not(own_first)
        my_in = jnp.where(is_first, cin, cin_second)
        my_out = jnp.where(is_first, cout_first, cout)
        if w == 0:
            x, g = xo_ref[:, cols].astype(F32), go_ref[:, cols].astype(F32)
            intra, dt_wide, te_wide, xw, gw = [own_refs[i][:, cols] for i in (1, 3, 4, 5, 6)]
        else:
            x, g = xgr_ref[0], xgr_ref[1]
            intra, dt_wide, te_wide, xw, gw = [rcv_refs[i][...] for i in (1, 3, 4, 5, 6)]
        b, c = packs[w][:, :state], packs[w][:, state : 2 * state]
        front = dot3(c, my_in, NN)
        back = dot3(b, my_out, NN)
        back_in = intra + te_wide * back
        grad_x = dt_wide * back_in + skip_wide * g
        if w == 0:
            gxo_ref[...] = grad_x.astype(BF16)
        else:
            gxs_ref[...] = grad_x
        sums.append([dot_left_full(v, collect, NN) for v in (x * back_in, gw * front)])
        gb.append(dot3(xw, my_out, NT))
        gc.append(dot3(gw, my_in, NT))
        ends.append(decays[w] * jnp.sum(my_in * my_out, axis=0, keepdims=True) + jnp.sum(xw * back, axis=0, keepdims=True))
        skips = skips + jnp.sum(x * g, axis=0, keepdims=True)
    row = iota((8, lanes), 0)
    stacked = jnp.where(row == 0, ends[0], jnp.where(row == 1, ends[1], jnp.where(row == 2, skips, 0.0)))
    small = dot_left_full(stacked, collect, NN)
    if chunk[0]:
        gb = [gb[w] + gbc_in_ref[w, :, :state] for w in (0, 1)]
        gc = [gc[w] + gbc_in_ref[w, :, state:] for w in (0, 1)]
        sums = [[sums[w][i] + sums_in_ref[w, i] for i in range(2)] for w in (0, 1)]
        small = small + small_in_ref[...]
    if not last:
        for w in (0, 1):
            gbc_ref[w, :, :state] = gb[w]
            gbc_ref[w, :, state:] = gc[w]
            for i in range(2):
                sums_ref[w, i] = sums[w][i]
        small_ref[...] = small
        return
    rate = misc_ref[0:1]
    later = triangle(length, False)
    last_row = iota((length, LANES), 0) == length - 1
    bias_sum = jnp.zeros((1, LANES), F32)
    alog_sum = jnp.zeros((1, LANES), F32)
    lane = iota((length, LANES), 1) < half
    block = pk_ref.shape[0] // 2 - 4
    for w, top in ((0, block), (1, 0)):
        tile = packs[w][:, 2 * state :]
        dt = jnp.where(lane, tile, 0.0)
        sig = pltpu.roll(tile, LANES - 2 * heads, 1)
        direct, ahead = sums[w]
        intra_rows = (rows_own_ref, rows_rcv_ref)[w]
        change = jnp.transpose(intra_rows[...]) + ahead - dt * direct
        change = change + jnp.where(last_row, small[w : w + 1], 0.0)
        grad_log = dot_right_full(later, change, NN)
        grad_raw = jnp.where(lane, (direct + grad_log * rate) * sig, 0.0)
        bias_sum = bias_sum + jnp.sum(grad_raw, axis=0, keepdims=True)
        alog_sum = alog_sum + jnp.sum(grad_log * dt, axis=0, keepdims=True) * rate
        intra_gbc = (gbc_own_ref, gbc_rcv_ref)[w]
        pk_ref[top : top + length] = gb[w] + intra_gbc[:, :state]
        pk_ref[top + length : top + 2 * length] = gc[w] + intra_gbc[:, state:]
        pk_ref[top + 2 * length : top + block] = folded(grad_raw)
    row = iota((8, LANES), 0)
    extra = jnp.where(row == 0, bias_sum, jnp.where(row == 1, alog_sum, jnp.where(row == 2, small[2:3], 0.0)))
    extra = jnp.where(iota((8, LANES), 1) < half, extra, 0.0)
    pk_ref[2 * block :] = pltpu.roll(extra, half * at_ref[0], 1)


def join_kernel(at_ref, own_ref, rcv_ref, out_ref, extra_ref, *, heads, length):
    half = heads // 2
    at = at_ref[0]
    block = own_ref.shape[0] // 2 - 4
    raws = []
    for w, (mine, other) in enumerate(((block, 0), (0, block))):
        out_ref[0, 2 * w * length : 2 * (w + 1) * length] = (
            own_ref[mine : mine + 2 * length] + rcv_ref[other : other + 2 * length]
        )
        kept = unfolded(own_ref[mine + 2 * length : mine + block])
        came = unfolded(rcv_ref[other + 2 * length : other + block])
        raws.append(pltpu.roll(kept, half * at, 1) + pltpu.roll(came, half * (1 - at), 1))
    out_ref[0, 4 * length :] = raws[0] + pltpu.roll(raws[1], LANES // 2, 1)
    extra_ref[...] = own_ref[2 * block :] + rcv_ref[2 * block :]


def merge_kernel(at_ref, *refs, chunks):
    out_ref = refs[-1]
    half_lanes = out_ref.shape[1] // 2
    for i, (start, lanes) in enumerate(chunks):
        mine = pl.multiple_of(at_ref[0] * half_lanes + start, LANES)
        other = pl.multiple_of((1 - at_ref[0]) * half_lanes + start, LANES)
        out_ref[:, pl.ds(mine, lanes)] = refs[i][...]
        out_ref[:, pl.ds(other, lanes)] = refs[len(chunks) + i][...].astype(BF16)


def grad_u_kernel(cols_ref, wb_ref, wc_ref, wd_ref, out_ref):
    length = out_ref.shape[0]
    total = dot_left(cols_ref[0, :length], wb_ref[...], NT)
    total = total + dot_left(cols_ref[0, length : 2 * length], wc_ref[...], NT)
    total = total + dot_left(cols_ref[0, 4 * length :], wd_ref[...], NN)
    out_ref[...] = total.astype(BF16)


def weight_kernel(at_ref, *refs, levels, pieces, heads):
    u_refs, col_refs = refs[:2], refs[2 : 2 + pieces]
    extra_ref, outs, all_ref = refs[2 + pieces], refs[3 + pieces : -1], refs[-1]
    u = jnp.concatenate([r[0, i].astype(BF16) for r in u_refs for i in range(pieces)], axis=0)
    length = u_refs[0].shape[2]
    each = (all_ref.shape[1] - heads) // 2
    row_sets = ([], [], [])
    low = iota((length, LANES), 1) < LANES // 2
    for w in range(2):
        for ref in col_refs:
            row_sets[0].append(ref[0, 2 * w * length : (2 * w + 1) * length])
            row_sets[1].append(ref[0, (2 * w + 1) * length : (2 * w + 2) * length])
            raw = ref[0, 4 * length :]
            row_sets[2].append(jnp.where(low, pltpu.roll(raw, LANES // 2, 1) if w else raw, 0.0))
    gb, gc, raw = [jnp.concatenate(v, axis=0) for v in row_sets]
    hi, lo = split2(jnp.concatenate([gb, gc], axis=1))
    wide = mm(u, hi, TN) + mm(u, lo, TN)
    state = gb.shape[1]
    thi, tlo = split2(raw)
    turned = (mm(thi, u, TN) + mm(tlo, u, TN))[:heads]
    turned = jnp.concatenate([turned, jnp.zeros((heads, LANES), F32)], axis=1)
    tail = jnp.transpose(jnp.concatenate([extra_ref[...], jnp.zeros((LANES - 8, LANES), F32)], axis=0))
    tail = pltpu.roll(tail, each, 1)[:heads]
    lane = iota((heads, LANES), 1)
    for s in range(levels):
        rows = slice(s * each, (s + 1) * each)
        all_ref[s, :each] = wide[rows, :state]
        all_ref[s, each : 2 * each] = wide[rows, state:]
        start = s * each // LANES * LANES
        window = pltpu.roll(turned[:, start : start + 2 * LANES], (2 * LANES + start - s * each) % (2 * LANES), 1)
        all_ref[s, 2 * each :] = jnp.where(lane < each, window[:, :LANES], tail)
    for k in range(levels):
        outs[k][0] = all_ref[jnp.bitwise_xor(at_ref[3], k)]


def final_kernel(at_ref, *refs, pieces, heads, order):
    parts = [r[i] for r in refs[:pieces] for i in range(r.shape[0])]
    gb_ref, gc_ref, gd_ref, bias_ref, alog_ref, skip_ref = refs[pieces:]
    rows_out = gb_ref.shape[0]
    each = rows_out // len(parts)
    mine = at_ref[2]
    total, wide = 0.0, 0.0
    around = -(-rows_out // LANES) * LANES + LANES
    for d in range(len(parts)):
        block = parts[0]
        for part, flip in list(zip(parts, order))[1:]:
            block = jnp.where(mine == d ^ flip, part, block)
        rows = slice(d * each, (d + 1) * each)
        gb_ref[rows] = block[:each]
        gc_ref[rows] = block[each : 2 * each]
        tail = block[2 * each :]
        total = total + tail
        tail = jnp.where(iota(tail.shape, 1) < each, tail, 0.0)
        tail = jnp.concatenate([tail, jnp.zeros((heads, around - LANES), F32)], axis=1)
        wide = wide + (pltpu.roll(tail, d * each, 1) if d else tail)
    gd_ref[...] = wide[:, :rows_out]
    total = jnp.concatenate([total, jnp.zeros((LANES - heads, LANES), F32)], axis=0)
    turned = jnp.transpose(total)
    bias_ref[...] = turned[each : each + 1, :heads]
    alog_ref[...] = turned[each + 1 : each + 2, :heads]
    skip_ref[...] = turned[each + 2 : each + 3, :heads]


def vmem(n):
    return [pl.BlockSpec(memory_space=pltpu.VMEM) for _ in range(n)]


def call(kernel, args, outs, scratch=(), scalars=None, flops=10**8, stay=False):
    specs = [pl.BlockSpec(memory_space=pltpu.HBM) for _ in args] if stay else vmem(len(args))
    if scalars is not None:
        specs, args = [pl.BlockSpec(memory_space=pltpu.SMEM)] + specs, [scalars, *args]
    return pl.pallas_call(
        kernel,
        in_specs=specs,
        out_specs=vmem(len(outs)),
        out_shape=[jax.ShapeDtypeStruct(s, t) for s, t in outs],
        scratch_shapes=list(scratch),
        cost_estimate=pl.CostEstimate(flops=flops, transcendentals=0, bytes_accessed=10**6),
        compiler_params=pltpu.CompilerParams(vmem_limit_bytes=12 << 20),
    )(*args)


def chunk_list(half, width):
    pairs = half * width // LANES
    whole = sum(SHARES)
    ends = [round(pairs * sum(SHARES[: i + 1]) / whole) for i in range(len(SHARES))]
    starts = [0] + ends[:-1]
    return [(a * LANES, (b - a) * LANES) for a, b in zip(starts, ends) if b > a]


def body(layer_input, ssm_input, out_grad, b_weight, c_weight, dt_weight, dt_bias, a_log, d_skip):
    length, model = layer_input.shape
    heads = dt_bias.shape[0]
    state = b_weight.shape[1]
    width = ssm_input.shape[1] // heads
    half = heads // 2
    lanes = half * width
    chunks = chunk_list(half, width)
    final = len(chunks) - 1
    count = lax.axis_size("seq")
    where = lax.axis_index("seq")
    place = where % 2
    level = where // 2
    levels = count // 2
    groups = lax.axis_size("dp")
    group = lax.axis_index("dp")
    each = model // count // groups
    bits = []
    while groups >> (len(bits) + 1):
        bits.insert(0, 1 << len(bits))
    at = lax.optimization_barrier(jnp.stack([place, level % 2, group, level]).astype(jnp.int32))
    swap = [(i, i ^ 1) for i in range(count)]
    rounds = []
    for r in range(levels - 1):
        far = levels - 1 - r
        rounds.append([p for i in range(2) for p in ((2 * r + i, 2 * r + 2 + i), (2 * far + i, 2 * far - 2 + i))])
    pack = 2 * state + LANES

    def exchange(value):
        return lax.ppermute(value, "seq", swap)

    def spread_pieces(value):
        pieces = [value]
        for bit in bits:
            pairs = [(d, d ^ bit) for d in range(groups)]
            for piece in list(pieces):
                pieces.append(lax.ppermute(piece, "dp", pairs))
        return pieces

    def halved(pieces, which, bit):
        targets, rows_each, cols_each = pieces[0].shape[0], pieces[0].shape[2], pieces[0].shape[3]
        shape = (targets // 2, sum(p.shape[1] for p in pieces), rows_each, cols_each)
        return call(
            functools.partial(halve_kernel, which=which, bit=bit), pieces,
            [(shape, BF16), (shape, F32)], scalars=at,
        )

    def column_pieces(value):
        room = -(levels * each) % LANES
        if each % 16 == 0 and groups > 1:
            shape = (groups, 1, length, levels * each + room)
            keep, sent = call(
                functools.partial(columns_kernel, levels=levels, groups=groups, each=each),
                [value], [(shape, BF16), (shape, F32)], scalars=at,
            )
        else:
            value = value.reshape(length, levels, 2, groups, each).transpose(3, 2, 0, 1, 4)
            value = value.reshape(2 * groups, 1, length, levels * each)
            value = jnp.pad(value, ((0, 0), (0, 0), (0, 0), (0, room)))
            keep, sent = halved([value], 2, max(groups // 2, 1))
        for i, bit in enumerate(bits):
            if i:
                keep, sent = halved([keep, came], 2, bit)
            came = lax.ppermute(sent, "dp", [(d, d ^ bit) for d in range(groups)])
        keep, sent = halved([keep, came], 0, 1)
        return [keep, exchange(sent)]

    x_far = pltpu.with_memory_space_constraint(ssm_input, pltpu.HBM)
    g_far = pltpu.with_memory_space_constraint(out_grad, pltpu.HBM)
    (sent,) = call(
        functools.partial(send_kernel, half_lanes=lanes, start=0), [x_far, g_far],
        [((2, length, chunks[0][1]), F32)], scalars=at, stay=True,
        scratch=[pltpu.VMEM((2, length, chunks[0][1]), BF16), pltpu.SemaphoreType.DMA((2,))],
    )
    received = [exchange(sent)]
    wd = jnp.pad(dt_weight.T, ((0, LANES - heads), (0, 0)))
    rows = jnp.pad(jnp.stack([dt_bias, a_log, d_skip]), ((0, 5), (0, LANES - heads)))
    own, send, misc = call(
        functools.partial(proj_kernel, heads=heads),
        [layer_input, b_weight, c_weight, wd, rows],
        [((length, pack), F32)] * 2 + [((8, LANES), F32)], scalars=at,
    )
    rcv = exchange(send)
    x_own, g_own, *sent = call(
        functools.partial(keep_kernel, half_lanes=lanes, chunks=chunks[1:]), [x_far, g_far],
        [((length, lanes), BF16)] * 2 + [((2, length, c[1]), F32) for c in chunks[1:]], scalars=at, stay=True,
        scratch=[
            pltpu.VMEM((2, length, max(lanes - chunks[0][1], LANES)), BF16),
            pltpu.SemaphoreType.DMA((2,)),
            pltpu.SemaphoreType.DMA((2,)),
        ],
    )
    send, *sent = lax.optimization_barrier((send, *sent))
    received += [exchange(v) for v in sent]
    u_pieces = column_pieces(layer_input)

    full = ((length, lanes), F32)
    back_own, gbc_own, rows_own, s_own, b_own, *own_rest = call(
        functools.partial(own_kernel, heads=heads, width=width), [x_own, g_own, own],
        [full, ((length, 2 * state), F32), ((LANES, length), F32), ((state, lanes), F32), ((state, lanes), F32)]
        + [((8, lanes), F32)] + [full] * 4,
        scratch=[pltpu.VMEM((LANES, length), F32), pltpu.VMEM((length, length), F32)], flops=10**9,
    )
    mine_all = [own, back_own, *own_rest]
    acc = rows_sum = None
    sums = []
    gx_own, gx_rcv = [], []
    for j, chunk in enumerate(chunks):
        last = j == final
        wide, tall = ((state, chunk[1]), F32), ((length, chunk[1]), F32)
        even, odd, s_first, g_second, decay, *rest = call(
            functools.partial(state_kernel, heads=heads, width=width, chunk=chunk),
            [received[j], rcv, s_own, b_own, own_rest[0]],
            [wide] * 4 + [((8, chunk[1]), F32)] * 2 + [tall] * 4, scalars=at,
        )
        decay = decay[:1]
        came = []
        for r, pairs in enumerate(rounds):
            value = (even, odd)[r % 2]
            if r:
                value = value + decay * came[-1]
            came.append(lax.ppermute(value, "seq", pairs))
        now, before = came[::-1][::2], came[::-1][1::2]
        if not before:
            before = [jnp.zeros((state, chunk[1]), F32)]
        if not now:
            now = before
        back, acc, rows_sum = call(
            functools.partial(intra_kernel, heads=heads, width=width, chunk=chunk, last=last),
            [received[j], rcv] + ([acc, rows_sum] if j else []),
            [tall, ((length, 2 * state if last else length), F32), ((LANES, length), F32)],
            scratch=[pltpu.VMEM((length, chunk[1]), BF16)] * 2 + [pltpu.VMEM((LANES, length), F32)]
            + ([pltpu.VMEM((length, length), F32)] if last else []),
            flops=10**9,
        )
        outs = [((length, chunk[1]), BF16), tall]
        if last:
            outs += [((2 * (2 * length + length * FOLD // LANES) + 8, LANES), F32)]
        else:
            outs += [((2, length, 2 * state), F32), ((2, 2, length, LANES), F32), ((8, LANES), F32)]
        mine, theirs, *sums = call(
            functools.partial(
                carry_kernel, heads=heads, width=width, chunk=chunk, last=last, came=(len(now), len(before))
            ),
            [*now, *before, s_first, g_second, misc, x_own, g_own, received[j]]
            + mine_all + [rcv, back, *rest] + sums
            + ([gbc_own, acc, rows_own, rows_sum] if last else []),
            outs, scalars=at,
        )
        gx_own.append(mine)
        if last:
            (pack_own,) = sums
            pack_rcv = exchange(pack_own)
        gx_rcv.append(exchange(theirs))
    cols, extra = call(
        functools.partial(join_kernel, heads=heads, length=length), [pack_own, pack_rcv],
        [((1, 5 * length, LANES), F32), ((8, LANES), F32)], scalars=at,
    )
    gathered = spread_pieces(cols)
    (grad_u,) = call(grad_u_kernel, [cols, b_weight, c_weight, wd], [((length, model), BF16)])
    (grad_x,) = call(
        functools.partial(merge_kernel, chunks=chunks), [*gx_own, *gx_rcv],
        [((length, 2 * lanes), BF16)], scalars=at,
    )
    block = ((1, 2 * each + heads, LANES), F32)
    blocks = call(
        functools.partial(weight_kernel, levels=levels, pieces=len(gathered), heads=heads),
        [*u_pieces, *gathered, extra], [block] * levels, scalars=at,
        scratch=[pltpu.VMEM((levels, *block[0][1:]), F32)],
    )
    moved = [blocks[0]]
    for k in range(1, levels):
        moved.append(lax.ppermute(blocks[k], "seq", [(i, i ^ (2 * k)) for i in range(count)]))
    (moved,) = call(total_kernel, moved, [block])
    parts = spread_pieces(moved)
    order = [0]
    for bit in bits:
        order = order + [f ^ bit for f in order]
    rows_out = model // count
    gb, gc, gd, bias, alog, skip = call(
        functools.partial(final_kernel, pieces=len(parts), heads=heads, order=order), parts,
        [((rows_out, state), F32)] * 2 + [((heads, rows_out), F32)] + [((1, heads), F32)] * 3, scalars=at,
    )
    return grad_x, grad_u, gb, gc, gd.T, bias[0], alog[0], skip[0]


def solution(mesh):
    rows = P(("dp", "seq"), None)
    in_specs = (rows, rows, rows, P(), P(), P(), P(), P(), P())
    out_specs = (rows, rows, P("seq", None), P("seq", None), P("seq", None), P(), P(), P())
    return jax.shard_map(body, mesh=mesh, in_specs=in_specs, out_specs=out_specs, check_vma=False)
```

```python
import functools

import jax
import jax.numpy as jnp
from jax import lax
from jax.experimental import pallas as pl
from jax.experimental.pallas import tpu as pltpu
from jax.sharding import PartitionSpec as P


F32 = jnp.float32
BF16 = jnp.bfloat16
LANES = 128
SHARES = (8, 8, 4)

NN = (((1,), (0,)), ((), ()))
NT = (((1,), (1,)), ((), ()))
TN = (((0,), (0,)), ((), ()))


def mm(a, b, dims):
    return lax.dot_general(a, b, dims, preferred_element_type=F32)


def split2(a):
    hi = a.astype(BF16)
    return hi, (a - hi.astype(F32)).astype(BF16)


def split3(a):
    hi = a.astype(BF16)
    rest = a - hi.astype(F32)
    mid = rest.astype(BF16)
    return hi, mid, (rest - mid.astype(F32)).astype(BF16)


def mm_sum(terms, dims):
    (left,), (right,) = dims[0]
    a = jnp.concatenate([t[0] for t in terms], axis=left)
    b = jnp.concatenate([t[1] for t in terms], axis=right)
    return mm(a, b, dims)


def dot3(a, b, dims):
    ah, al = split2(a)
    bh, bl = split2(b)
    return mm_sum([(al, bh), (ah, bl), (ah, bh)], dims)


def dot_left(a, b, dims):
    ah, al = split2(a)
    return mm_sum([(al, b), (ah, b)], dims)


def dot_left_full(a, b, dims):
    ah, am, al = split3(a)
    return mm_sum([(al, b), (am, b), (ah, b)], dims)


def dot_right_full(a, b, dims):
    bh, bm, bl = split3(b)
    return mm_sum([(a, bl), (a, bm), (a, bh)], dims)


def iota(shape, axis):
    return lax.broadcasted_iota(jnp.int32, shape, axis)


def log1p_unit(y):
    s = y / (2.0 + y)
    q = s * s
    poly = jnp.full_like(q, 1.0 / 17)
    for k in (15, 13, 11, 9, 7, 5, 3, 1):
        poly = poly * q + 1.0 / k
    return 2.0 * s * poly


def triangle(length, lower):
    r, c = iota((length, length), 0), iota((length, length), 1)
    keep = (r >= c) if lower else (c >= r)
    return jnp.where(keep, 1.0, 0.0).astype(BF16)


def expand_matrix(head_start, width, lanes):
    r, c = iota((LANES, lanes), 0), iota((LANES, lanes), 1)
    return jnp.where(r == head_start + c // width, 1.0, 0.0).astype(BF16)


def collect_matrix(head_start, width, lanes):
    r, c = iota((lanes, LANES), 0), iota((lanes, LANES), 1)
    return jnp.where(c == head_start + r // width, 1.0, 0.0).astype(BF16)


def coefficients(tile, heads_all, heads_half):
    lane = iota(tile.shape, 1) < heads_half
    length = tile.shape[0]
    dt = jnp.where(lane, tile, 0.0)
    cum = jnp.where(lane, pltpu.roll(tile, LANES - heads_all, 1), 0.0)
    last = cum[length - 1 : length, :]
    from_start = jnp.where(lane, jnp.exp(cum), 0.0)
    to_end = jnp.where(lane, jnp.exp(last - cum), 0.0)
    decay = jnp.where(lane[:1], jnp.exp(last), 0.0)
    return dt, cum, from_start, to_end, decay


def row_of(v, rows=8):
    return jnp.broadcast_to(v, (rows, v.shape[1]))


def lanes_of(chunk):
    return slice(chunk[0], chunk[0] + chunk[1])


def send_kernel(at_ref, x_ref, g_ref, out_ref, buf_ref, sems, *, half_lanes, start):
    part = out_ref.shape[2]
    first = pl.multiple_of((1 - at_ref[0]) * half_lanes + start, LANES)
    copies = []
    for i, ref in enumerate((x_ref, g_ref)):
        copies.append(pltpu.make_async_copy(ref.at[:, pl.ds(first, part)], buf_ref.at[i], sems.at[i]))
        copies[-1].start()
    for i, copy in enumerate(copies):
        copy.wait()
        out_ref[i] = buf_ref[i].astype(F32)


def keep_kernel(at_ref, x_ref, g_ref, *refs, half_lanes, chunks):
    keeps, sends = refs[:2], refs[2 : 2 + len(chunks)]
    buf_ref, keep_sems, send_sems = refs[2 + len(chunks) :]
    own = pl.multiple_of(at_ref[0] * half_lanes, LANES)
    other = pl.multiple_of((1 - at_ref[0]) * half_lanes, LANES)
    rest = half_lanes - chunks[0][0] if chunks else 0
    sending, keeping = [], []
    for i, ref in enumerate((x_ref, g_ref)):
        if chunks:
            source = ref.at[:, pl.ds(pl.multiple_of(other + chunks[0][0], LANES), rest)]
            sending.append(pltpu.make_async_copy(source, buf_ref.at[i], send_sems.at[i]))
            sending[-1].start()
        keeping.append(pltpu.make_async_copy(ref.at[:, pl.ds(own, half_lanes)], keeps[i], keep_sems.at[i]))
        keeping[-1].start()
    for i, copy in enumerate(sending):
        copy.wait()
        for chunk, out_ref in zip(chunks, sends):
            first = chunk[0] - chunks[0][0]
            out_ref[i] = buf_ref[i, :, first : first + chunk[1]].astype(F32)
    for copy in keeping:
        copy.wait()


def columns_kernel(at_ref, u_ref, keep_ref, send_ref, *, levels, groups, each):
    u = u_ref[...].astype(F32)
    taken = []
    for d in range(groups):
        for p in range(2):
            starts = [((2 * z + p) * groups + d) * each for z in range(levels)]
            parts = [u[:, a : a + each] for a in starts]
            room = keep_ref.shape[3] - levels * each
            taken.append(jnp.concatenate(parts + [jnp.zeros((u.shape[0], room), F32)] * (room > 0), axis=1))
    half = groups
    high = at_ref[2] >= groups // 2
    for i in range(half):
        keep_ref[i, 0] = jnp.where(high, taken[half + i], taken[i]).astype(BF16)
        send_ref[i, 0] = jnp.where(high, taken[i], taken[half + i])


def halve_kernel(at_ref, *refs, which, bit):
    keep_ref, send_ref = refs[-2:]
    high = (at_ref[which] // bit) % 2 == 1
    half = keep_ref.shape[0]
    done = 0
    for ref in refs[:-2]:
        for k in range(ref.shape[1]):
            for i in range(half):
                low_part, high_part = ref[i, k].astype(F32), ref[half + i, k].astype(F32)
                keep_ref[i, done + k] = jnp.where(high, high_part, low_part).astype(BF16)
                send_ref[i, done + k] = jnp.where(high, low_part, high_part)
        done += ref.shape[1]


def total_kernel(*refs):
    total = refs[0][...]
    for ref in refs[1:-1]:
        total = total + ref[...]
    refs[-1][...] = total


FOLD = 32


def folded(tile):
    rows = tile.shape[0] // (LANES // FOLD)
    lane = iota((rows, LANES), 1) // FOLD
    out = tile[:rows]
    for q in range(1, LANES // FOLD):
        out = jnp.where(lane == q, pltpu.roll(tile[q * rows : (q + 1) * rows], q * FOLD, 1), out)
    return out


def unfolded(tile):
    parts = [tile] + [pltpu.roll(tile, LANES - q * FOLD, 1) for q in range(1, LANES // FOLD)]
    out = jnp.concatenate(parts, axis=0)
    return jnp.where(iota(out.shape, 1) < FOLD, out, 0.0)


def proj_kernel(at_ref, u_ref, wb_ref, wc_ref, wd_ref, rows_ref, own_ref, snd_ref, misc_ref, *, heads):
    length = u_ref.shape[0]
    state = wb_ref.shape[1]
    u = u_ref[...]
    b = mm(u, wb_ref[...], NN)
    c = mm(u, wc_ref[...], NN)
    raw = mm(u, wd_ref[...], NT) + rows_ref[0:1]
    dt = jnp.maximum(raw, 0.0) + log1p_unit(jnp.exp(-jnp.abs(raw)))
    sig = 1.0 / (1.0 + jnp.exp(-raw))
    rate = -jnp.exp(rows_ref[1:2])
    cum = dot_right_full(triangle(length, True), dt * rate, NN)
    lane = iota(raw.shape, 1)
    tile = jnp.where(
        lane < heads,
        dt,
        jnp.where(lane < 2 * heads, pltpu.roll(cum, heads, 1), pltpu.roll(sig, 2 * heads, 1)),
    )
    half = heads // 2
    at = at_ref[0]
    mine = (LANES - half * at) % LANES
    for ref, shift in ((own_ref, mine), (snd_ref, (LANES - half * (1 - at)) % LANES)):
        ref[:, :state] = b
        ref[:, state : 2 * state] = c
        ref[:, 2 * state :] = pltpu.roll(tile, shift, 1)
    row = iota((8, LANES), 0)
    both = jnp.where(row == 0, jnp.broadcast_to(rate, (8, LANES)), rows_ref[...])
    misc_ref[...] = pltpu.roll(both, mine, 1)


def local_states(x, g, pack_ref, heads, width, start):
    half = heads // 2
    state = (pack_ref.shape[1] - LANES) // 2
    spread = expand_matrix(start, width, x.shape[1])
    dt, _, from_start, to_end, decay = coefficients(pack_ref[:, 2 * state :], heads, half)
    dt_wide = dot_left(dt, spread, NN)
    te_wide = dot_left(to_end, spread, NN)
    xw = x * (dt_wide * te_wide)
    gw = g * dot_left(from_start, spread, NN)
    s = dot3(pack_ref[:, :state], xw, TN)
    back = dot3(pack_ref[:, state : 2 * state], gw, TN)
    return s, back, dot_left_full(row_of(decay), spread, NN), dt_wide, te_wide, xw, gw


def intra_pairs(x_ref, g_ref, tile, scores, cumt_ref, acc_ref, rows_ref, back_ref, heads, width, pair0, pairs, unroll):
    length = scores.shape[0]
    src, dst = iota((length, length), 0), iota((length, length), 1)
    causal = dst >= src
    low = iota((length, LANES), 1) < width

    def step(k, _):
        at = pl.multiple_of(k * LANES, LANES)
        xp = x_ref[:, pl.ds(at, LANES)]
        gp = g_ref[:, pl.ds(at, LANES)]
        zero = jnp.zeros_like(xp)
        x2 = jnp.concatenate([jnp.where(low, xp, zero), jnp.where(low, zero, xp)], axis=0)
        g2 = jnp.concatenate([jnp.where(low, gp, zero), jnp.where(low, zero, gp)], axis=0)
        dots = mm(x2, gp, NT)
        turned = pltpu.roll(tile, LANES - 2 * (k + pair0), 1)
        his, los = [], []
        total = 0.0
        for e in range(2):
            h = 2 * (k + pair0) + e
            dt_col = jnp.broadcast_to(turned[:, e : e + 1], (length, length))
            cum_col = jnp.broadcast_to(turned[:, heads + e : heads + e + 1], (length, length))
            cum_row = cumt_ref[pl.ds(h, 1), :]
            table = jnp.exp(jnp.where(causal, cum_row - cum_col, -1e30))
            both = table * dots[e * length : (e + 1) * length] * dt_col
            total = total + both
            rows_ref[pl.ds(h, 1), :] = jnp.sum(both * scores, axis=0, keepdims=True)
            hi, lo = split2(table * scores)
            his.append(hi)
            los.append(lo)
        acc_ref[...] += total
        back_ref[:, pl.ds(at, LANES)] = mm_sum(
            [(jnp.concatenate(los, axis=1), g2), (jnp.concatenate(his, axis=1), g2)], NN
        )
        return 0

    lax.fori_loop(0, pairs, step, 0, unroll=unroll)


def own_kernel(
    xo_ref, go_ref, po_ref, back_ref, gbc_ref, rows_ref, s_ref, b_ref, d_ref, dt_ref, te_ref, xw_ref, gw_ref,
    cumt_ref, acc_ref, *, heads, width,
):
    state = (po_ref.shape[1] - LANES) // 2
    b = po_ref[:, :state]
    c = po_ref[:, state : 2 * state]
    tile = po_ref[:, 2 * state :]
    cumt_ref[...] = jnp.transpose(pltpu.roll(tile, LANES - heads, 1))
    acc_ref[...] = jnp.zeros_like(acc_ref)
    rows_ref[...] = jnp.zeros_like(rows_ref)
    intra_pairs(
        xo_ref, go_ref, tile, dot3(b, c, NT), cumt_ref, acc_ref, rows_ref, back_ref,
        heads, width, 0, xo_ref.shape[1] // LANES, 2,
    )
    acc = acc_ref[...]
    gbc_ref[:, :state] = dot3(acc, c, NN)
    gbc_ref[:, state:] = dot3(acc, b, TN)
    outs = local_states(xo_ref[...].astype(F32), go_ref[...].astype(F32), po_ref, heads, width, 0)
    for ref, value in zip((s_ref, b_ref, d_ref, dt_ref, te_ref, xw_ref, gw_ref), outs):
        ref[...] = value


def state_kernel(
    at_ref, xgr_ref, pr_ref, s_ref, b_ref, d_ref,
    even_ref, odd_ref, sf_ref, gs_ref, dp_ref, dr_ref, dt_ref, te_ref, xw_ref, gw_ref, *, heads, width, chunk,
):
    first_is_own = at_ref[0] == 0
    even = at_ref[1] == 0
    cols = lanes_of(chunk)
    s_own, b_own, d_own = s_ref[:, cols], b_ref[:, cols], d_ref[:, cols]
    s_rcv, b_rcv, d_rcv, *rest = local_states(xgr_ref[0], xgr_ref[1], pr_ref, heads, width, chunk[0] // width)

    def pick(a, b):
        return jnp.where(first_is_own, a, b)

    s_first, s_second = pick(s_own, s_rcv), pick(s_rcv, s_own)
    b_first, b_second = pick(b_own, b_rcv), pick(b_rcv, b_own)
    d_first, d_second = pick(d_own, d_rcv), pick(d_rcv, d_own)
    p = d_second[:1] * s_first + s_second
    q = d_first[:1] * b_second + b_first
    even_ref[...] = jnp.where(even, p, q)
    odd_ref[...] = jnp.where(even, q, p)
    sf_ref[...] = s_first
    gs_ref[...] = b_second
    dp_ref[...] = d_first * d_second
    dr_ref[...] = d_rcv
    for ref, value in zip((dt_ref, te_ref, xw_ref, gw_ref), rest):
        ref[...] = value


def intra_kernel(xgr_ref, pr_ref, *refs, heads, width, chunk, last):
    if chunk[0]:
        acc_in_ref, rows_in_ref, *refs = refs
    if last:
        back_ref, gbc_ref, rows_ref, x_ref, g_ref, cumt_ref, acc_ref = refs
    else:
        back_ref, acc_ref, rows_ref, x_ref, g_ref, cumt_ref = refs
    state = (pr_ref.shape[1] - LANES) // 2
    b = pr_ref[:, :state]
    c = pr_ref[:, state : 2 * state]
    tile = pr_ref[:, 2 * state :]
    x_ref[...] = xgr_ref[0].astype(BF16)
    g_ref[...] = xgr_ref[1].astype(BF16)
    cumt_ref[...] = jnp.transpose(pltpu.roll(tile, LANES - heads, 1))
    acc_ref[...] = acc_in_ref[...] if chunk[0] else jnp.zeros(acc_ref.shape, F32)
    rows_ref[...] = rows_in_ref[...] if chunk[0] else jnp.zeros(rows_ref.shape, F32)
    intra_pairs(
        x_ref, g_ref, tile, dot3(b, c, NT), cumt_ref, acc_ref, rows_ref, back_ref,
        heads, width, chunk[0] // LANES, chunk[1] // LANES, True,
    )
    if last:
        acc = acc_ref[...]
        gbc_ref[:, :state] = dot3(acc, c, NN)
        gbc_ref[:, state:] = dot3(acc, b, TN)


def carry_kernel(at_ref, *refs, heads, width, chunk, last, came):
    now = sum(ref[...] for ref in refs[: came[0]])
    before = sum(ref[...] for ref in refs[came[0] : sum(came)])
    refs = refs[sum(came) :]
    sf_ref, gs_ref, misc_ref, xo_ref, go_ref, xgr_ref, *refs = refs
    own_refs, rcv_refs, refs = refs[:7], refs[7:14], refs[14:]
    if chunk[0]:
        gbc_in_ref, sums_in_ref, small_in_ref, *refs = refs
    if last:
        gbc_own_ref, gbc_rcv_ref, rows_own_ref, rows_rcv_ref, *refs = refs
        gxo_ref, gxs_ref, pk_ref = refs
    else:
        gxo_ref, gxs_ref, gbc_ref, sums_ref, small_ref = refs
    half = heads // 2
    lanes = chunk[1]
    cols = lanes_of(chunk)
    own_first = at_ref[0] == 0
    even = at_ref[1] == 0
    packs = (own_refs[0], rcv_refs[0])
    length = packs[0].shape[0]
    state = (packs[0].shape[1] - LANES) // 2
    spread = expand_matrix(chunk[0] // width, width, lanes)
    collect = collect_matrix(chunk[0] // width, width, lanes)
    skip_row = jnp.where(iota((1, LANES), 1) < half, misc_ref[2:3], 0.0)
    skip_wide = dot_left_full(row_of(skip_row), spread, NN)[:1]
    decays = (own_refs[2][:1, cols], rcv_refs[2][:1])
    cin, cout = jnp.where(even, before, now), jnp.where(even, now, before)
    d_first = jnp.where(own_first, decays[0], decays[1])
    d_second = jnp.where(own_first, decays[1], decays[0])
    cin_second = d_first * cin + sf_ref[...]
    cout_first = d_second * cout + gs_ref[...]
    gb, gc, sums, ends, skips = [], [], [], [], 0.0
    for w in (0, 1):
        is_first = own_first if w == 0 else jnp.logical_not(own_first)
        my_in = jnp.where(is_first, cin, cin_second)
        my_out = jnp.where(is_first, cout_first, cout)
        if w == 0:
            x, g = xo_ref[:, cols].astype(F32), go_ref[:, cols].astype(F32)
            intra, dt_wide, te_wide, xw, gw = [own_refs[i][:, cols] for i in (1, 3, 4, 5, 6)]
        else:
            x, g = xgr_ref[0], xgr_ref[1]
            intra, dt_wide, te_wide, xw, gw = [rcv_refs[i][...] for i in (1, 3, 4, 5, 6)]
        b, c = packs[w][:, :state], packs[w][:, state : 2 * state]
        front = dot3(c, my_in, NN)
        back = dot3(b, my_out, NN)
        back_in = intra + te_wide * back
        grad_x = dt_wide * back_in + skip_wide * g
        if w == 0:
            gxo_ref[...] = grad_x.astype(BF16)
        else:
            gxs_ref[...] = grad_x
        sums.append([x * back_in, gw * front])
        gb.append(dot3(xw, my_out, NT))
        gc.append(dot3(gw, my_in, NT))
        ends.append(decays[w] * jnp.sum(my_in * my_out, axis=0, keepdims=True) + jnp.sum(xw * back, axis=0, keepdims=True))
        skips = skips + jnp.sum(x * g, axis=0, keepdims=True)
    joint = dot_left(jnp.concatenate([v for both in sums for v in both], axis=0), collect, NN)
    sums = [[joint[(2 * w + i) * length : (2 * w + i + 1) * length] for i in range(2)] for w in (0, 1)]
    row = iota((8, lanes), 0)
    stacked = jnp.where(row == 0, ends[0], jnp.where(row == 1, ends[1], jnp.where(row == 2, skips, 0.0)))
    small = dot_left_full(stacked, collect, NN)
    if chunk[0]:
        gb = [gb[w] + gbc_in_ref[w, :, :state] for w in (0, 1)]
        gc = [gc[w] + gbc_in_ref[w, :, state:] for w in (0, 1)]
        sums = [[sums[w][i] + sums_in_ref[w, i] for i in range(2)] for w in (0, 1)]
        small = small + small_in_ref[...]
    if not last:
        for w in (0, 1):
            gbc_ref[w, :, :state] = gb[w]
            gbc_ref[w, :, state:] = gc[w]
            for i in range(2):
                sums_ref[w, i] = sums[w][i]
        small_ref[...] = small
        return
    rate = misc_ref[0:1]
    later = triangle(length, False)
    last_row = iota((length, LANES), 0) == length - 1
    bias_sum = jnp.zeros((1, LANES), F32)
    alog_sum = jnp.zeros((1, LANES), F32)
    lane = iota((length, LANES), 1) < half
    block = pk_ref.shape[0] // 2 - 4
    for w, top in ((0, block), (1, 0)):
        tile = packs[w][:, 2 * state :]
        dt = jnp.where(lane, tile, 0.0)
        sig = pltpu.roll(tile, LANES - 2 * heads, 1)
        direct, ahead = sums[w]
        intra_rows = (rows_own_ref, rows_rcv_ref)[w]
        change = jnp.transpose(intra_rows[...]) + ahead - dt * direct
        change = change + jnp.where(last_row, small[w : w + 1], 0.0)
        grad_log = dot_right_full(later, change, NN)
        grad_raw = jnp.where(lane, (direct + grad_log * rate) * sig, 0.0)
        bias_sum = bias_sum + jnp.sum(grad_raw, axis=0, keepdims=True)
        alog_sum = alog_sum + jnp.sum(grad_log * dt, axis=0, keepdims=True) * rate
        intra_gbc = (gbc_own_ref, gbc_rcv_ref)[w]
        pk_ref[top : top + length] = gb[w] + intra_gbc[:, :state]
        pk_ref[top + length : top + 2 * length] = gc[w] + intra_gbc[:, state:]
        pk_ref[top + 2 * length : top + block] = folded(grad_raw)
    row = iota((8, LANES), 0)
    extra = jnp.where(row == 0, bias_sum, jnp.where(row == 1, alog_sum, jnp.where(row == 2, small[2:3], 0.0)))
    extra = jnp.where(iota((8, LANES), 1) < half, extra, 0.0)
    pk_ref[2 * block :] = pltpu.roll(extra, half * at_ref[0], 1)


def join_kernel(at_ref, own_ref, rcv_ref, out_ref, extra_ref, *, heads, length):
    half = heads // 2
    at = at_ref[0]
    block = own_ref.shape[0] // 2 - 4
    raws = []
    for w, (mine, other) in enumerate(((block, 0), (0, block))):
        out_ref[0, 2 * w * length : 2 * (w + 1) * length] = (
            own_ref[mine : mine + 2 * length] + rcv_ref[other : other + 2 * length]
        )
        kept = unfolded(own_ref[mine + 2 * length : mine + block])
        came = unfolded(rcv_ref[other + 2 * length : other + block])
        raws.append(pltpu.roll(kept, half * at, 1) + pltpu.roll(came, half * (1 - at), 1))
    out_ref[0, 4 * length :] = raws[0] + pltpu.roll(raws[1], LANES // 2, 1)
    extra_ref[...] = own_ref[2 * block :] + rcv_ref[2 * block :]


def merge_kernel(at_ref, *refs, chunks):
    out_ref = refs[-1]
    half_lanes = out_ref.shape[1] // 2
    for i, (start, lanes) in enumerate(chunks):
        mine = pl.multiple_of(at_ref[0] * half_lanes + start, LANES)
        other = pl.multiple_of((1 - at_ref[0]) * half_lanes + start, LANES)
        out_ref[:, pl.ds(mine, lanes)] = refs[i][...]
        out_ref[:, pl.ds(other, lanes)] = refs[len(chunks) + i][...].astype(BF16)


def grad_u_kernel(cols_ref, wb_ref, wc_ref, wd_ref, out_ref):
    length = out_ref.shape[0]
    total = dot_left(cols_ref[0, :length], wb_ref[...], NT)
    total = total + dot_left(cols_ref[0, length : 2 * length], wc_ref[...], NT)
    total = total + dot_left(cols_ref[0, 4 * length :], wd_ref[...], NN)
    out_ref[...] = total.astype(BF16)


def turn_kernel(*refs):
    out_ref = refs[-1]
    length = refs[0].shape[2]
    done = 0
    for ref in refs[:-1]:
        for i in range(ref.shape[1]):
            out_ref[:, done : done + length] = jnp.transpose(ref[0, i].astype(F32)).astype(BF16)
            done += length


def weight_kernel(at_ref, u_ref, *refs, levels, pieces, heads):
    col_refs, extra_ref, outs, all_ref = refs[:pieces], refs[pieces], refs[pieces + 1 : -1], refs[-1]
    length = u_ref.shape[1] // (2 * pieces)
    each = (all_ref.shape[1] - heads) // 2
    row_sets = ([], [], [])
    low = iota((length, LANES), 1) < LANES // 2
    for w in range(2):
        for ref in col_refs:
            row_sets[0].append(ref[0, 2 * w * length : (2 * w + 1) * length])
            row_sets[1].append(ref[0, (2 * w + 1) * length : (2 * w + 2) * length])
            raw = ref[0, 4 * length :]
            row_sets[2].append(jnp.where(low, pltpu.roll(raw, LANES // 2, 1) if w else raw, 0.0))
    hi, lo = split2(jnp.concatenate([jnp.concatenate(v, axis=0) for v in row_sets], axis=1))
    u = u_ref[...]
    wide = mm(u, hi, NN) + mm(u, lo, NN)
    state = (wide.shape[1] - LANES) // 2
    turned = jnp.transpose(wide[:, 2 * state :])[:heads]
    wide = wide[:, : 2 * state]
    turned = jnp.concatenate([turned, jnp.zeros((heads, LANES), F32)], axis=1)
    tail = jnp.transpose(jnp.concatenate([extra_ref[...], jnp.zeros((LANES - 8, LANES), F32)], axis=0))
    tail = pltpu.roll(tail, each, 1)[:heads]
    lane = iota((heads, LANES), 1)
    for s in range(levels):
        rows = slice(s * each, (s + 1) * each)
        all_ref[s, :each] = wide[rows, :state]
        all_ref[s, each : 2 * each] = wide[rows, state:]
        start = s * each // LANES * LANES
        window = pltpu.roll(turned[:, start : start + 2 * LANES], (2 * LANES + start - s * each) % (2 * LANES), 1)
        all_ref[s, 2 * each :] = jnp.where(lane < each, window[:, :LANES], tail)
    for k in range(levels):
        outs[k][0] = all_ref[jnp.bitwise_xor(at_ref[3], k)]


def final_kernel(at_ref, *refs, pieces, heads, order):
    parts = [r[i] for r in refs[:pieces] for i in range(r.shape[0])]
    gb_ref, gc_ref, gd_ref, bias_ref, alog_ref, skip_ref = refs[pieces:]
    rows_out = gb_ref.shape[0]
    each = rows_out // len(parts)
    mine = at_ref[2]
    total, wide = 0.0, 0.0
    around = -(-rows_out // LANES) * LANES + LANES
    for d in range(len(parts)):
        block = parts[0]
        for part, flip in list(zip(parts, order))[1:]:
            block = jnp.where(mine == d ^ flip, part, block)
        rows = slice(d * each, (d + 1) * each)
        gb_ref[rows] = block[:each]
        gc_ref[rows] = block[each : 2 * each]
        tail = block[2 * each :]
        total = total + tail
        tail = jnp.where(iota(tail.shape, 1) < each, tail, 0.0)
        tail = jnp.concatenate([tail, jnp.zeros((heads, around - LANES), F32)], axis=1)
        wide = wide + (pltpu.roll(tail, d * each, 1) if d else tail)
    gd_ref[...] = wide[:, :rows_out]
    total = jnp.concatenate([total, jnp.zeros((LANES - heads, LANES), F32)], axis=0)
    turned = jnp.transpose(total)
    bias_ref[...] = turned[each : each + 1, :heads]
    alog_ref[...] = turned[each + 1 : each + 2, :heads]
    skip_ref[...] = turned[each + 2 : each + 3, :heads]


def vmem(n):
    return [pl.BlockSpec(memory_space=pltpu.VMEM) for _ in range(n)]


def call(kernel, args, outs, scratch=(), scalars=None, flops=10**8, stay=False):
    specs = [pl.BlockSpec(memory_space=pltpu.HBM) for _ in args] if stay else vmem(len(args))
    if scalars is not None:
        specs, args = [pl.BlockSpec(memory_space=pltpu.SMEM)] + specs, [scalars, *args]
    return pl.pallas_call(
        kernel,
        in_specs=specs,
        out_specs=vmem(len(outs)),
        out_shape=[jax.ShapeDtypeStruct(s, t) for s, t in outs],
        scratch_shapes=list(scratch),
        cost_estimate=pl.CostEstimate(flops=flops, transcendentals=0, bytes_accessed=10**6),
        compiler_params=pltpu.CompilerParams(vmem_limit_bytes=12 << 20),
    )(*args)


def chunk_list(half, width):
    pairs = half * width // LANES
    whole = sum(SHARES)
    ends = [round(pairs * sum(SHARES[: i + 1]) / whole) for i in range(len(SHARES))]
    starts = [0] + ends[:-1]
    return [(a * LANES, (b - a) * LANES) for a, b in zip(starts, ends) if b > a]


def body(layer_input, ssm_input, out_grad, b_weight, c_weight, dt_weight, dt_bias, a_log, d_skip):
    length, model = layer_input.shape
    heads = dt_bias.shape[0]
    state = b_weight.shape[1]
    width = ssm_input.shape[1] // heads
    half = heads // 2
    lanes = half * width
    chunks = chunk_list(half, width)
    final = len(chunks) - 1
    count = lax.axis_size("seq")
    where = lax.axis_index("seq")
    place = where % 2
    level = where // 2
    levels = count // 2
    groups = lax.axis_size("dp")
    group = lax.axis_index("dp")
    each = model // count // groups
    bits = []
    while groups >> (len(bits) + 1):
        bits.insert(0, 1 << len(bits))
    at = lax.optimization_barrier(jnp.stack([place, level % 2, group, level]).astype(jnp.int32))
    swap = [(i, i ^ 1) for i in range(count)]
    rounds = []
    for r in range(levels - 1):
        far = levels - 1 - r
        rounds.append([p for i in range(2) for p in ((2 * r + i, 2 * r + 2 + i), (2 * far + i, 2 * far - 2 + i))])
    pack = 2 * state + LANES

    def exchange(value):
        return lax.ppermute(value, "seq", swap)

    def spread_pieces(value):
        pieces = [value]
        for bit in bits:
            pairs = [(d, d ^ bit) for d in range(groups)]
            for piece in list(pieces):
                pieces.append(lax.ppermute(piece, "dp", pairs))
        return pieces

    def halved(pieces, which, bit):
        targets, rows_each, cols_each = pieces[0].shape[0], pieces[0].shape[2], pieces[0].shape[3]
        shape = (targets // 2, sum(p.shape[1] for p in pieces), rows_each, cols_each)
        return call(
            functools.partial(halve_kernel, which=which, bit=bit), pieces,
            [(shape, BF16), (shape, F32)], scalars=at,
        )

    def column_pieces(value):
        room = -(levels * each) % LANES
        if each % 16 == 0 and groups > 1:
            shape = (groups, 1, length, levels * each + room)
            keep, sent = call(
                functools.partial(columns_kernel, levels=levels, groups=groups, each=each),
                [value], [(shape, BF16), (shape, F32)], scalars=at,
            )
        else:
            value = value.reshape(length, levels, 2, groups, each).transpose(3, 2, 0, 1, 4)
            value = value.reshape(2 * groups, 1, length, levels * each)
            value = jnp.pad(value, ((0, 0), (0, 0), (0, 0), (0, room)))
            keep, sent = halved([value], 2, max(groups // 2, 1))
        for i, bit in enumerate(bits):
            if i:
                keep, sent = halved([keep, came], 2, bit)
            came = lax.ppermute(sent, "dp", [(d, d ^ bit) for d in range(groups)])
        keep, sent = halved([keep, came], 0, 1)
        return [keep, exchange(sent)]

    x_far = pltpu.with_memory_space_constraint(ssm_input, pltpu.HBM)
    g_far = pltpu.with_memory_space_constraint(out_grad, pltpu.HBM)
    (sent,) = call(
        functools.partial(send_kernel, half_lanes=lanes, start=0), [x_far, g_far],
        [((2, length, chunks[0][1]), F32)], scalars=at, stay=True,
        scratch=[pltpu.VMEM((2, length, chunks[0][1]), BF16), pltpu.SemaphoreType.DMA((2,))],
    )
    received = [exchange(sent)]
    wd = jnp.pad(dt_weight.T, ((0, LANES - heads), (0, 0)))
    rows = jnp.pad(jnp.stack([dt_bias, a_log, d_skip]), ((0, 5), (0, LANES - heads)))
    own, send, misc = call(
        functools.partial(proj_kernel, heads=heads),
        [layer_input, b_weight, c_weight, wd, rows],
        [((length, pack), F32)] * 2 + [((8, LANES), F32)], scalars=at,
    )
    rcv = exchange(send)
    x_own, g_own, *sent = call(
        functools.partial(keep_kernel, half_lanes=lanes, chunks=chunks[1:]), [x_far, g_far],
        [((length, lanes), BF16)] * 2 + [((2, length, c[1]), F32) for c in chunks[1:]], scalars=at, stay=True,
        scratch=[
            pltpu.VMEM((2, length, max(lanes - chunks[0][1], LANES)), BF16),
            pltpu.SemaphoreType.DMA((2,)),
            pltpu.SemaphoreType.DMA((2,)),
        ],
    )
    send, *sent = lax.optimization_barrier((send, *sent))
    received += [exchange(v) for v in sent]
    u_pieces = column_pieces(layer_input)

    full = ((length, lanes), F32)
    back_own, gbc_own, rows_own, s_own, b_own, *own_rest = call(
        functools.partial(own_kernel, heads=heads, width=width), [x_own, g_own, own],
        [full, ((length, 2 * state), F32), ((LANES, length), F32), ((state, lanes), F32), ((state, lanes), F32)]
        + [((8, lanes), F32)] + [full] * 4,
        scratch=[pltpu.VMEM((LANES, length), F32), pltpu.VMEM((length, length), F32)], flops=10**9,
    )
    mine_all = [own, back_own, *own_rest]
    acc = rows_sum = None
    sums = []
    gx_own, gx_rcv = [], []
    for j, chunk in enumerate(chunks):
        last = j == final
        wide, tall = ((state, chunk[1]), F32), ((length, chunk[1]), F32)
        even, odd, s_first, g_second, decay, *rest = call(
            functools.partial(state_kernel, heads=heads, width=width, chunk=chunk),
            [received[j], rcv, s_own, b_own, own_rest[0]],
            [wide] * 4 + [((8, chunk[1]), F32)] * 2 + [tall] * 4, scalars=at,
        )
        decay = decay[:1]
        came = []
        for r, pairs in enumerate(rounds):
            value = (even, odd)[r % 2]
            if r:
                value = value + decay * came[-1]
            came.append(lax.ppermute(value, "seq", pairs))
        now, before = came[::-1][::2], came[::-1][1::2]
        if not before:
            before = [jnp.zeros((state, chunk[1]), F32)]
        if not now:
            now = before
        back, acc, rows_sum = call(
            functools.partial(intra_kernel, heads=heads, width=width, chunk=chunk, last=last),
            [received[j], rcv] + ([acc, rows_sum] if j else []),
            [tall, ((length, 2 * state if last else length), F32), ((LANES, length), F32)],
            scratch=[pltpu.VMEM((length, chunk[1]), BF16)] * 2 + [pltpu.VMEM((LANES, length), F32)]
            + ([pltpu.VMEM((length, length), F32)] if last else []),
            flops=10**9,
        )
        outs = [((length, chunk[1]), BF16), tall]
        if last:
            outs += [((2 * (2 * length + length * FOLD // LANES) + 8, LANES), F32)]
        else:
            outs += [((2, length, 2 * state), F32), ((2, 2, length, LANES), F32), ((8, LANES), F32)]
        mine, theirs, *sums = call(
            functools.partial(
                carry_kernel, heads=heads, width=width, chunk=chunk, last=last, came=(len(now), len(before))
            ),
            [*now, *before, s_first, g_second, misc, x_own, g_own, received[j]]
            + mine_all + [rcv, back, *rest] + sums
            + ([gbc_own, acc, rows_own, rows_sum] if last else []),
            outs, scalars=at,
        )
        gx_own.append(mine)
        if last:
            (pack_own,) = sums
            pack_rcv = exchange(pack_own)
        gx_rcv.append(exchange(theirs))
    cols, extra = call(
        functools.partial(join_kernel, heads=heads, length=length), [pack_own, pack_rcv],
        [((1, 5 * length, LANES), F32), ((8, LANES), F32)], scalars=at,
    )
    gathered = spread_pieces(cols)
    (u_turned,) = call(
        turn_kernel, u_pieces,
        [((u_pieces[0].shape[3], 2 * groups * length), BF16)],
    )
    (grad_u,) = call(grad_u_kernel, [cols, b_weight, c_weight, wd], [((length, model), BF16)])
    (grad_x,) = call(
        functools.partial(merge_kernel, chunks=chunks), [*gx_own, *gx_rcv],
        [((length, 2 * lanes), BF16)], scalars=at,
    )
    block = ((1, 2 * each + heads, LANES), F32)
    blocks = call(
        functools.partial(weight_kernel, levels=levels, pieces=len(gathered), heads=heads),
        [u_turned, *gathered, extra], [block] * levels, scalars=at,
        scratch=[pltpu.VMEM((levels, *block[0][1:]), F32)],
    )
    moved = [blocks[0]]
    for k in range(1, levels):
        moved.append(lax.ppermute(blocks[k], "seq", [(i, i ^ (2 * k)) for i in range(count)]))
    (moved,) = call(total_kernel, moved, [block])
    parts = spread_pieces(moved)
    order = [0]
    for bit in bits:
        order = order + [f ^ bit for f in order]
    rows_out = model // count
    gb, gc, gd, bias, alog, skip = call(
        functools.partial(final_kernel, pieces=len(parts), heads=heads, order=order), parts,
        [((rows_out, state), F32)] * 2 + [((heads, rows_out), F32)] + [((1, heads), F32)] * 3, scalars=at,
    )
    return grad_x, grad_u, gb, gc, gd.T, bias[0], alog[0], skip[0]


def solution(mesh):
    rows = P(("dp", "seq"), None)
    in_specs = (rows, rows, rows, P(), P(), P(), P(), P(), P())
    out_specs = (rows, rows, P("seq", None), P("seq", None), P("seq", None), P(), P(), P())
    return jax.shard_map(body, mesh=mesh, in_specs=in_specs, out_specs=out_specs, check_vma=False)
```
